32 devices in a mesh: dp: 4 (over y, z), sp: 8 (over x, core).
Axes of the slice: x: 4, y: 2, z: 2, core: 2. Of those that a mesh axis runs over, the one named last changes fastest.
The devices are a block of a 4x4x8 slice.
Arguments:
- hidden: bfloat16 [12288, 3072], P(('dp', 'sp')), parts along dimension 0
- positions: int32 [12288], P(('dp', 'sp')), parts along dimension 0
- norm_gain: bfloat16 [3072], replicated
- w_q: bfloat16 [3072, 3072], replicated
- b_q: bfloat16 [3072], replicated
- w_k: bfloat16 [3072, 1024], replicated
- b_k: bfloat16 [1024], replicated
- w_v: bfloat16 [3072, 1024], replicated
- b_v: bfloat16 [1024], replicated
- w_o: bfloat16 [3072, 3072], replicated
Outputs:
- output 1: bfloat16 [12288, 3072], P(('dp', 'sp')), parts along dimension 0
- output 2: bfloat16 [12288, 8, 128], P('dp', 'sp'), parts along dimension 0
- output 3: bfloat16 [12288, 8, 128], P('dp', 'sp'), parts along dimension 0
There are 4 independent parts. The reference program is written for one: setup_inputs(seed, part) draws one part's arguments, and reference() takes and returns one part's arrays. A program takes and returns all parts, laid end to end along the dimension named above; an argument that names none is the same for every part.
All inputs are finite; a program needn't handle non-finite values.
Results may differ from the reference program's by a relative error of at most 0.00856746.
Values are sent between devices in bfloat16 or wider.
A program may use at most 768 MiB of HBM per device.

```python
import jax
import jax.numpy as jnp
from jax import lax

MODEL_DIM = 3072
Q_HEADS = 24
KV_HEADS = 8
HEAD_DIM = 128
SEQ_LEN = 3072
SEG_COUNT = 16
QUERY_BLOCK = 64

ROPE_BASE = 1000000.0
NORM_EPS = 1e-6
Q_WIDTH = Q_HEADS * HEAD_DIM
KV_WIDTH = KV_HEADS * HEAD_DIM
GROUP_REP = Q_HEADS // KV_HEADS


def draw_normal(key, shape, scale):
    return (scale * jax.random.normal(key, shape, jnp.float32)).astype(jnp.bfloat16)


def setup_inputs(seed: int = 0, part: int = 0) -> dict:
    part_keys = jax.random.split(jax.random.fold_in(jax.random.key(seed), part), 4)
    shared = jax.random.split(jax.random.key(seed + 1), 10)
    offsets = jax.random.normal(part_keys[0], (SEG_COUNT, MODEL_DIM), jnp.float32)
    noise = jax.random.normal(part_keys[1], (SEQ_LEN, MODEL_DIM), jnp.float32)
    hidden = 0.5 * jnp.repeat(offsets, SEQ_LEN // SEG_COUNT, axis=0) + 0.25 * noise
    start = jax.random.randint(part_keys[2], (), 0, 4096, jnp.int32)
    gaps = jax.random.randint(part_keys[3], (SEQ_LEN,), 1, 3, jnp.int32)
    positions = start + jnp.cumsum(gaps) - gaps[0]
    norm_gain = 1.0 + 0.3 * jax.random.normal(shared[0], (MODEL_DIM,), jnp.float32)
    return {
        'hidden': hidden.astype(jnp.bfloat16),
        'positions': positions.astype(jnp.int32),
        'norm_gain': norm_gain.astype(jnp.bfloat16),
        'w_q': draw_normal(shared[1], (MODEL_DIM, Q_WIDTH), 1.5 * MODEL_DIM ** -0.5),
        'b_q': draw_normal(shared[2], (Q_WIDTH,), 0.5),
        'w_k': draw_normal(shared[3], (MODEL_DIM, KV_WIDTH), MODEL_DIM ** -0.5),
        'b_k': draw_normal(shared[4], (KV_WIDTH,), 0.5),
        'w_v': draw_normal(shared[5], (MODEL_DIM, KV_WIDTH), MODEL_DIM ** -0.5),
        'b_v': draw_normal(shared[6], (KV_WIDTH,), 0.5),
        'w_o': draw_normal(shared[7], (Q_WIDTH, MODEL_DIM), Q_WIDTH ** -0.5),
    }


def rms_norm(hidden, norm_gain):
    wide = hidden.astype(jnp.float32)
    inv_rms = lax.rsqrt(jnp.mean(wide * wide, axis=-1, keepdims=True) + NORM_EPS)
    return (wide * inv_rms * norm_gain.astype(jnp.float32)).astype(jnp.bfloat16)


def project(normed, weight, bias):
    summed = jnp.dot(normed, weight, preferred_element_type=jnp.float32)
    return (summed + bias.astype(jnp.float32)).astype(jnp.bfloat16)


def apply_rope(heads, positions):
    half_dim = HEAD_DIM // 2
    inv_freq = ROPE_BASE ** (-2.0 * jnp.arange(half_dim, dtype=jnp.float32) / HEAD_DIM)
    angle = positions.astype(jnp.float32)[:, None, None] * inv_freq
    cosine = jnp.cos(angle)
    sine = jnp.sin(angle)
    wide = heads.astype(jnp.float32)
    lower = wide[..., :half_dim]
    upper = wide[..., half_dim:]
    turned = jnp.concatenate([lower * cosine - upper * sine, upper * cosine + lower * sine], axis=-1)
    return turned.astype(jnp.bfloat16)


def reference(hidden, positions, norm_gain, w_q, b_q, w_k, b_k, w_v, b_v, w_o):
    normed = rms_norm(hidden, norm_gain)
    queries = apply_rope(project(normed, w_q, b_q).reshape(SEQ_LEN, Q_HEADS, HEAD_DIM), positions)
    keys = apply_rope(project(normed, w_k, b_k).reshape(SEQ_LEN, KV_HEADS, HEAD_DIM), positions)
    values = project(normed, w_v, b_v).reshape(SEQ_LEN, KV_HEADS, HEAD_DIM)
    grouped = queries.reshape(SEQ_LEN, KV_HEADS, GROUP_REP, HEAD_DIM)
    keys_wide = keys.astype(jnp.float32)
    values_wide = values.astype(jnp.float32)
    key_index = jnp.arange(SEQ_LEN)
    scale = HEAD_DIM ** -0.5

    def one_block(block_id):
        first = block_id * QUERY_BLOCK
        q_block = lax.dynamic_slice_in_dim(grouped, first, QUERY_BLOCK, axis=0).astype(jnp.float32)
        scores = jnp.einsum('qgrd,kgd->qgrk', q_block, keys_wide) * scale
        row_index = first + jnp.arange(QUERY_BLOCK)
        allowed = row_index[:, None, None, None] >= key_index[None, None, None, :]
        scores = jnp.where(allowed, scores, -jnp.inf)
        weights = jax.nn.softmax(scores, axis=-1).astype(jnp.bfloat16)
        mixed = jnp.einsum('qgrk,kgd->qgrd', weights.astype(jnp.float32), values_wide)
        return mixed.astype(jnp.bfloat16)

    attended = lax.map(one_block, jnp.arange(SEQ_LEN // QUERY_BLOCK)).reshape(SEQ_LEN, Q_WIDTH)
    summed = hidden.astype(jnp.float32) + jnp.dot(attended, w_o, preferred_element_type=jnp.float32)
    return summed.astype(jnp.bfloat16), keys, values
```

```python
import functools
import math

import jax
import jax.numpy as jnp
from jax import lax
from jax.experimental import pallas as pl
from jax.experimental.pallas import tpu as pltpu
from jax.sharding import PartitionSpec as P

HEAD_DIM = 128
ROPE_BASE = 1000000.0
NORM_EPS = 1e-6
SCORE_SCALE = math.log2(math.e) / math.sqrt(HEAD_DIM)
CHIPS = 4
GROUPS = 4
REPS = 3
TILE = 256
BF16 = jnp.bfloat16
F32 = jnp.float32


def rope_tables(positions):
    half_dim = HEAD_DIM // 2
    inv_freq = ROPE_BASE ** (-2.0 * jnp.arange(half_dim, dtype=F32) / HEAD_DIM)
    angle = positions.astype(F32)[:, None] * inv_freq
    cosine = jnp.cos(angle)
    sine = jnp.sin(angle)
    return jnp.concatenate([cosine, cosine], axis=-1), jnp.concatenate([-sine, sine], axis=-1)


def matmul(a, b):
    return lax.dot_general(a, b, (((1,), (0,)), ((), ())), preferred_element_type=F32)


def matmul_t(a, b):
    return lax.dot_general(a, b, (((1,), (1,)), ((), ())), preferred_element_type=F32)


def lane_blocks(x):
    return [x[:, i : i + 128] for i in range(0, x.shape[1], 128)]


def pipelined(count, score, soft, mix):
    scores, weights = {}, {}
    for t in range(count + 2):
        if t < count:
            scores[t] = score(t)
        if 0 <= t - 1 < count:
            weights[t - 1] = soft(t - 1, scores.pop(t - 1))
        if 0 <= t - 2 < count:
            mix(t - 2, *weights.pop(t - 2))


def kernel(
    x_hbm, cos_ref, sin_ref, gain_ref, bq_ref, bk_ref, bv_ref, wq_hbm, wk_hbm, wv_hbm, wo_hbm,
    y_hbm, kc_hbm, vc_hbm,
    xbuf, hbuf, wkv, wbuf, kv, kst, qbuf, qst, run_max, run_sum, mixed, obuf, ost,
    xsem, wkvsem, wqsem, wosem, ysem, csem,
    kv_recv, kv_send, q_recv, q_send, o_recv, o_send, fwd_send,
):
    me = lax.axis_index("sp")
    chip = lax.div(me, 2)
    core = lax.rem(me, 2)
    other = 1 - core
    up = lax.rem(chip + 1, CHIPS)
    down = lax.rem(chip + CHIPS - 1, CHIPS)
    tokens = xbuf.shape[0]
    block = 2 * tokens
    my_rows = pl.ds(pl.multiple_of(core * tokens, 128), tokens)
    other_rows = pl.ds(pl.multiple_of(other * tokens, 128), tokens)

    def is_chip(n):
        return chip == n

    def device(on_chip, on_core):
        return {"sp": on_chip * 2 + on_core}

    def remote(src, dst, send_sem, recv_sem, on_chip, on_core):
        return pltpu.make_async_remote_copy(
            src_ref=src, dst_ref=dst, send_sem=send_sem, recv_sem=recv_sem,
            device_id=device(on_chip, on_core), device_id_type=pl.DeviceIdType.MESH,
        )

    barrier = pltpu.get_barrier_semaphore()
    for on_chip, on_core in ((chip, other), (up, core), (up, other), (down, core), (down, other)):
        pl.semaphore_signal(barrier, inc=1, device_id=device(on_chip, on_core), device_id_type=pl.DeviceIdType.MESH)

    first_group = jnp.where(chip == 0, 0, 1)

    def group_at(i):
        return lax.rem(i + first_group, GROUPS)

    def kv_load(chunk_i, kind):
        w_hbm = wk_hbm if kind == 0 else wv_hbm
        chunk = 2 * chunk_i + kind
        cols = pl.ds(pl.multiple_of(group_at(chunk_i) * 256, 256), 256)
        return pltpu.make_async_copy(w_hbm.at[:, cols], wkv.at[lax.rem(chunk, 4)], wkvsem.at[chunk])

    def wide_load(w_hbm, g, sem):
        cols = pl.ds(pl.multiple_of(g * 768, 256), 768)
        return pltpu.make_async_copy(w_hbm.at[:, cols], wbuf.at[g], sem.at[g])

    x_copy = pltpu.make_async_copy(x_hbm, xbuf, xsem)
    x_copy.start()
    for i in range(2):
        for kind in range(2):
            kv_load(jnp.int32(i), kind).start()
    x_copy.wait()

    @pl.loop(0, tokens // 32)
    def _(i):
        rows = pl.ds(pl.multiple_of(i * 32, 32), 32)
        wide = xbuf[rows, :].astype(F32)
        inv_rms = lax.rsqrt(jnp.mean(wide * wide, axis=-1, keepdims=True) + NORM_EPS)
        hbuf[rows, :] = (wide * inv_rms * gain_ref[...]).astype(BF16)

    pl.semaphore_wait(barrier, 5)

    def rope(u):
        wide = u.astype(F32)
        return (wide * cos_ref[...] + pltpu.roll(wide, HEAD_DIM // 2, 1) * sin_ref[...]).astype(BF16)

    def goes_partner(g):
        return jnp.logical_not((chip == 3) & (g == 0))

    def goes_up(g):
        return (chip <= 1) | ((chip == 2) & (g >= 1)) | ((chip == 3) & (g <= 1))

    def goes_down(g):
        return ((chip == 0) & (g >= 1)) | ((chip == 1) & ((g == 0) | (g == 3))) | ((chip == 2) & (g <= 1)) | ((chip == 3) & (g == 2))

    def own_copies(g):
        dst = kv.at[chip, g, :, my_rows, :]
        recv = kv_recv.at[chip, g, core]
        yield goes_partner(g), [remote(kst.at[g], dst, kv_send.at[g, 0], recv, chip, other)]
        yield goes_up(g), [
            remote(dst, dst, kv_send.at[g, 1], recv, up, core), remote(kst.at[g], dst, kv_send.at[g, 2], recv, up, other)]
        yield goes_down(g), [
            remote(dst, dst, kv_send.at[g, 3], recv, down, core), remote(kst.at[g], dst, kv_send.at[g, 4], recv, down, other)]

    def each(copies, act):
        for go, group in copies:
            @pl.when(go)
            def _():
                for copy in group:
                    act(copy)

    @pl.loop(0, GROUPS)
    def _(i):
        g = group_at(i)
        cols = pl.ds(pl.multiple_of(g * 256, 256), 256)
        for kind, b_ref in ((0, bk_ref), (1, bv_ref)):
            chunk = 2 * i + kind
            kv_load(i, kind).wait()
            u = (matmul(hbuf[...], wkv[lax.rem(chunk, 4)]) + b_ref[:, cols]).astype(BF16)
            even, odd = lane_blocks(u)
            if kind == 0:
                even, odd = rope(even), rope(odd)
            kv[chip, g, kind, my_rows, :] = jnp.where(core == 0, even, odd)
            kst[g, kind] = jnp.where(core == 0, odd, even)

            @pl.when(i < 2)
            def _():
                kv_load(i + 2, kind).start()

        wide_load(wq_hbm, i, wqsem).start()
        each(own_copies(g), lambda copy: copy.start())

    def q_copies(g):
        mine = qbuf.at[g, :, my_rows, :]
        away = (chip == 3) & (g == 0)
        yield jnp.logical_not(away), [
            remote(qst.at[g], mine, q_send.at[g, 0], q_recv.at[g, core], chip, other)]
        there = qbuf.at[GROUPS, :, my_rows, :]
        yield away, [
            remote(mine, there, q_send.at[g, 1], q_recv.at[GROUPS, core], up, core),
            remote(qst.at[g], there, q_send.at[g, 0], q_recv.at[GROUPS, core], up, other)]

    @pl.loop(0, GROUPS)
    def _(g):
        wide_load(wq_hbm, g, wqsem).wait()
        heads = []
        for n in range(3):
            cols = pl.ds(pl.multiple_of(g * 768 + n * 256, 256), 256)
            u = (matmul(hbuf[...], wbuf[g, :, n * 256 : (n + 1) * 256]) + bq_ref[:, cols]).astype(BF16)
            heads += [rope(part) for part in lane_blocks(u)]
        for r in range(REPS):
            even, odd = heads[r], heads[REPS + r]
            qbuf[g, r, my_rows, :] = jnp.where(core == 0, even, odd)
            qst[g, r] = jnp.where(core == 0, odd, even)
        wide_load(wo_hbm, g, wosem).start()
        each(q_copies(g), lambda copy: copy.start())

    def wait_straight(s, g):
        for j in range(2):
            part = kv.at[s, g, :, pl.ds(j * tokens, tokens), :]
            pltpu.make_async_copy(part, part, kv_recv.at[s, g, j]).wait()

    def wait_passed(s, g):
        pltpu.make_async_copy(kv.at[s, g], kv.at[s, g], kv_recv.at[s, g, 0]).wait()

    def pass_on(s, g, to_chip, slot):
        return remote(kv.at[s, g], kv.at[s, g], fwd_send.at[slot], kv_recv.at[s, g, 0], to_chip, core)

    q_tiles = block // TILE

    def tile_rows(t):
        return t // q_tiles, slice((t % q_tiles) * TILE, (t % q_tiles + 1) * TILE)

    def masked_item(q_slot, slot, s, g):
        def score(t):
            r, rows = tile_rows(t)
            sc = matmul_t(qbuf[q_slot, r, rows, :], kv[s, g, 0, 0 : rows.stop, :])
            seen = lax.broadcasted_iota(jnp.int32, (TILE, TILE), 0) >= lax.broadcasted_iota(jnp.int32, (TILE, TILE), 1)
            last = jnp.where(seen, sc[:, rows.start :], -jnp.inf)
            return last if rows.start == 0 else jnp.concatenate([sc[:, : rows.start], last], axis=1)

        def soft(t, sc):
            r, rows = tile_rows(t)
            parts = lane_blocks(sc)
            top = functools.reduce(jnp.maximum, parts)
            top = jnp.broadcast_to(jnp.max(top, axis=1, keepdims=True) * SCORE_SCALE, (TILE, 128))
            probs = [jnp.exp2(part * SCORE_SCALE - top) for part in parts]
            run_max[slot, r, rows, :] = top
            run_sum[slot, r, rows, :] = functools.reduce(jnp.add, probs)
            return (jnp.concatenate([p.astype(BF16) for p in probs], axis=1),)

        def mix(t, probs):
            r, rows = tile_rows(t)
            mixed[slot, r, rows, :] = matmul(probs, kv[s, g, 1, 0 : rows.stop, :])

        pipelined(REPS * q_tiles, score, soft, mix)

    def full_item(q_slot, slot, s, g):
        def score(t):
            r, rows = tile_rows(t)
            return matmul_t(qbuf[q_slot, r, rows, :], kv[s, g, 0])

        def soft(t, sc):
            r, rows = tile_rows(t)
            parts = lane_blocks(sc)
            before = run_max[slot, r, rows, :]
            top = functools.reduce(jnp.maximum, parts)
            top = jnp.maximum(before, jnp.max(top, axis=1, keepdims=True) * SCORE_SCALE)
            rescale = jnp.exp2(before - top)
            probs = [jnp.exp2(part * SCORE_SCALE - top) for part in parts]
            run_max[slot, r, rows, :] = top
            run_sum[slot, r, rows, :] = run_sum[slot, r, rows, :] * rescale + functools.reduce(jnp.add, probs)
            return jnp.concatenate([p.astype(BF16) for p in probs], axis=1), rescale

        def mix(t, probs, rescale):
            r, rows = tile_rows(t)
            mixed[slot, r, rows, :] = mixed[slot, r, rows, :] * rescale + matmul(probs, kv[s, g, 1])

        pipelined(REPS * q_tiles, score, soft, mix)

    def head_cols(g, parity):
        return pl.ds(pl.multiple_of((2 * g + parity) * REPS * 128, 128), REPS * 128)

    def normalized(slot, r, rows):
        total = jnp.sum(run_sum[slot, r, rows, :], axis=1, keepdims=True)
        return (mixed[slot, r, rows, :] / total).astype(BF16)

    def o_copy(g):
        return remote(ost.at[g], obuf.at[:, head_cols(g, core)], o_send.at[g], o_recv.at[g, core], chip, other)

    def finish(g):
        for r in range(REPS):
            ost[g, :, r * 128 : (r + 1) * 128] = normalized(g, r, other_rows)
        o_copy(g).start()
        for r in range(REPS):
            cols = pl.ds(pl.multiple_of(((2 * g + core) * REPS + r) * 128, 128), 128)
            obuf[:, cols] = normalized(g, r, my_rows)

    def back_copies():
        for j in range(2):
            yield remote(ost.at[GROUPS + j], obuf.at[:, head_cols(0, core)], o_send.at[GROUPS + j], o_recv.at[0, core], down, j)

    low = jnp.where(chip == 3, 1, 0)

    @pl.loop(low, jnp.where(chip == 0, GROUPS + 1, GROUPS))
    def _(i):
        g = lax.rem(i, GROUPS)

        @pl.when(i < GROUPS)
        def _():
            part = qbuf.at[i, :, other_rows, :]
            pltpu.make_async_copy(part, part, q_recv.at[i, other]).wait()
            part = kv.at[chip, g, :, other_rows, :]
            pltpu.make_async_copy(part, part, kv_recv.at[chip, g, other]).wait()

        @pl.when(i == GROUPS)
        def _():
            wait_straight(1, 3)
            pass_on(1, 3, 3, 0).start()
            wait_straight(3, 1)
            pass_on(3, 1, 1, 1).start()
            wait_straight(3, 0)
            for j in range(2):
                part = qbuf.at[GROUPS, :, pl.ds(j * tokens, tokens), :]
                pltpu.make_async_copy(part, part, q_recv.at[GROUPS, j]).wait()

        masked_item(i, g, jnp.where(i == GROUPS, 3, chip), g)

        @pl.when((chip == 0) & (i < GROUPS))
        def _():
            finish(i)

    straight = jnp.where(chip == 0, 3, jnp.where(chip == 3, 6, 4))
    items = straight + jnp.where(chip == 3, 3, jnp.where(chip == 2, 4, 0))

    @pl.loop(0, items)
    def _(i):
        late = i - straight
        in_order = lax.rem(i, GROUPS)
        shifted = lax.rem(i + 1, GROUPS)
        s = jnp.where(
            chip == 0, i,
            jnp.where(chip == 1, 0,
                jnp.where(chip == 2, jnp.where(late < 0, 1, 0), jnp.where(late < 0, 2 - 2 * lax.rem(i, 2), 1))))
        g = jnp.where(
            chip == 0, 0,
            jnp.where(chip == 1, in_order,
                jnp.where(chip == 2, shifted, jnp.where(late < 0, 1 + lax.div(i, 2), 1 + lax.rem(2 * late + 6, 3)))))
        q_slot = jnp.where(chip == 0, GROUPS, g)
        is_passed = ((chip == 0) & (i == 2)) | (late >= 0)
        is_local = (chip == 0) & (i == 0)

        @pl.when(is_passed)
        def _():
            wait_passed(s, g)

        @pl.when(jnp.logical_not(is_passed | is_local))
        def _():
            wait_straight(s, g)

        @pl.when((chip == 1) & (i == 0))
        def _():
            pass_on(0, 0, 2, 0).start()

        @pl.when((chip == 1) & (i == 1))
        def _():
            wait_straight(2, 0)
            pass_on(2, 0, 0, 1).start()

        @pl.when((chip == 2) & (late < 0) & ((g == 1) | (g == 2)))
        def _():
            pass_on(1, g, 3, g - 1).start()

        @pl.when((chip == 3) & (late < 0) & (s == 0))
        def _():
            pass_on(0, g, 2, g - 1).start()

        full_item(q_slot, g, s, g)

    @pl.when(chip == 0)
    def _():
        for j in range(2):
            rows = pl.ds(j * tokens, tokens)
            for r in range(REPS):
                ost[GROUPS + j, :, r * 128 : (r + 1) * 128] = normalized(0, r, rows)
        for copy in back_copies():
            copy.start()

    @pl.when(chip > 0)
    def _():
        @pl.loop(low, GROUPS)
        def _(g):
            finish(g)

    @pl.when(chip == 1)
    def _():
        wait_straight(2, 1)
        wait_passed(3, 1)

    @pl.when(chip == 2)
    def _():
        wait_straight(3, 2)

    cache_copies = []
    for s in range(CHIPS):
        for kind, c_hbm in ((0, kc_hbm), (1, vc_hbm)):
            cache_copies.append(
                pltpu.make_async_copy(kv.at[s, chip, kind], c_hbm.at[pl.ds(s * block, block), :], csem.at[s, kind]))
    for copy in cache_copies:
        copy.start()

    def wait_o(g, parity):
        part = obuf.at[:, head_cols(g, parity)]
        pltpu.make_async_copy(part, part, o_recv.at[g, parity]).wait()

    @pl.loop(low, GROUPS)
    def _(g):
        wait_o(g, other)

    @pl.when(chip == 3)
    def _():
        for parity in range(2):
            wait_o(0, parity)

    def y_copy(n):
        cols = pl.ds(pl.multiple_of(n * 768, 256), 768)
        return pltpu.make_async_copy(xbuf.at[:, cols], y_hbm.at[:, cols], ysem.at[n])

    @pl.loop(0, 4)
    def _(n):
        wide_load(wo_hbm, n, wosem).wait()
        for part in range(3):
            cols = pl.ds(pl.multiple_of(n * 768 + part * 256, 256), 256)
            summed = matmul(obuf[...], wbuf[n, :, part * 256 : (part + 1) * 256])
            xbuf[:, cols] = (xbuf[:, cols].astype(F32) + summed).astype(BF16)
        y_copy(n).start()

    @pl.loop(0, GROUPS)
    def _(g):
        each(own_copies(g), lambda copy: copy.wait_send())
        each(q_copies(g), lambda copy: copy.wait_send())

    @pl.loop(low, GROUPS)
    def _(g):
        o_copy(g).wait_send()

    @pl.when(chip == 0)
    def _():
        for copy in back_copies():
            copy.wait_send()

    for slot in range(2):
        pass_on(0, 0, up, slot).wait_send()

    @pl.when(chip == 3)
    def _():
        pass_on(0, 0, up, 2).wait_send()

    for copy in cache_copies:
        copy.wait()

    @pl.loop(0, 4)
    def _(n):
        y_copy(n).wait()


def solution(mesh):
    group_size = mesh.shape['sp']
    row_spec = P(('dp', 'sp'), None)
    pos_spec = P(('dp', 'sp'))
    cache_spec = P('dp', 'sp', None)
    whole = P()

    def local(hidden, positions, norm_gain, w_q, b_q, w_k, b_k, w_v, b_v, w_o):
        tokens, width = hidden.shape
        block = 2 * tokens
        seq_len = tokens * group_size
        cosine, sine = rope_tables(positions)
        vmem = pl.BlockSpec(memory_space=pltpu.VMEM)
        anywhere = pl.BlockSpec(memory_space=pl.ANY)
        dma = pltpu.SemaphoreType.DMA
        y, keys, values = pl.pallas_call(
            kernel,
            out_shape=[
                jax.ShapeDtypeStruct((tokens, width), BF16),
                jax.ShapeDtypeStruct((seq_len, HEAD_DIM), BF16),
                jax.ShapeDtypeStruct((seq_len, HEAD_DIM), BF16),
            ],
            in_specs=[anywhere] + [vmem] * 6 + [anywhere] * 4,
            out_specs=[anywhere] * 3,
            scratch_shapes=[
                pltpu.VMEM((tokens, width), BF16),
                pltpu.VMEM((tokens, width), BF16),
                pltpu.VMEM((4, width, 256), BF16),
                pltpu.VMEM((GROUPS, width, 768), BF16),
                pltpu.VMEM((CHIPS, GROUPS, 2, block, HEAD_DIM), BF16),
                pltpu.VMEM((GROUPS, 2, tokens, HEAD_DIM), BF16),
                pltpu.VMEM((GROUPS + 1, REPS, block, HEAD_DIM), BF16),
                pltpu.VMEM((GROUPS, REPS, tokens, HEAD_DIM), BF16),
                pltpu.VMEM((GROUPS, REPS, block, HEAD_DIM), F32),
                pltpu.VMEM((GROUPS, REPS, block, HEAD_DIM), F32),
                pltpu.VMEM((GROUPS, REPS, block, HEAD_DIM), F32),
                pltpu.VMEM((tokens, width), BF16),
                pltpu.VMEM((GROUPS + 2, tokens, REPS * HEAD_DIM), BF16),
                dma, dma((8,)), dma((4,)), dma((4,)), dma((4,)), dma((CHIPS, 2)),
                dma((CHIPS, GROUPS, 2)), dma((GROUPS, 5)), dma((GROUPS + 1, 2)), dma((GROUPS, 2)),
                dma((GROUPS, 2)), dma((GROUPS + 2,)), dma((3,)),
            ],
            compiler_params=pltpu.CompilerParams(
                collective_id=0, has_side_effects=True, vmem_limit_bytes=67043328),
            name="block",
        )(
            hidden, cosine, sine, norm_gain.astype(F32)[None], b_q.astype(F32)[None], b_k.astype(F32)[None],
            b_v.astype(F32)[None], w_q, w_k, w_v, w_o,
        )
        return y, keys[:, None, :], values[:, None, :]

    return jax.shard_map(local, mesh=mesh, in_specs=(row_spec, pos_spec, whole, whole, whole, whole, whole, whole, whole, whole), out_specs=(row_spec, cache_spec, cache_spec), check_vma=False)
```

```python
import functools
import math

import jax
import jax.numpy as jnp
from jax import lax
from jax.experimental import pallas as pl
from jax.experimental.pallas import tpu as pltpu
from jax.sharding import PartitionSpec as P

HEAD_DIM = 128
ROPE_BASE = 1000000.0
NORM_EPS = 1e-6
SCORE_SCALE = math.log2(math.e) / math.sqrt(HEAD_DIM)
CHIPS = 4
GROUPS = 4
REPS = 3
TILE = 256
BF16 = jnp.bfloat16
F32 = jnp.float32


def rope_tables(positions):
    half_dim = HEAD_DIM // 2
    inv_freq = ROPE_BASE ** (-2.0 * jnp.arange(half_dim, dtype=F32) / HEAD_DIM)
    angle = positions.astype(F32)[:, None] * inv_freq
    return jnp.cos(angle), jnp.sin(angle)


def matmul(a, b):
    return lax.dot_general(a, b, (((1,), (0,)), ((), ())), preferred_element_type=F32)


def matmul_t(a, b):
    return lax.dot_general(a, b, (((1,), (1,)), ((), ())), preferred_element_type=F32)


def matmul_halves(a_ref, b):
    half = a_ref.shape[0] // 2
    return jnp.concatenate([matmul(a_ref[:half], b), matmul(a_ref[half:], b)], axis=0)


def pick(i, values):
    out = values[-1]
    for n in range(len(values) - 1):
        out = jnp.where(i == n, values[n], out)
    return out


def lane_blocks(x):
    return [x[:, i : i + 128] for i in range(0, x.shape[1], 128)]


def pipelined(count, score, soft, mix):
    scores, weights = {}, {}
    for t in range(count + 2):
        if t < count:
            scores[t] = score(t)
        if 0 <= t - 1 < count:
            weights[t - 1] = soft(t - 1, scores.pop(t - 1))
        if 0 <= t - 2 < count:
            mix(t - 2, *weights.pop(t - 2))


def kernel(
    x_hbm, cos_hbm, sin_hbm, gain_hbm, bq_hbm, bk_hbm, bv_hbm, wq_hbm, wk_hbm, wv_hbm, wo_hbm,
    y_hbm, kc_hbm, vc_hbm,
    xbuf, hbuf, cos_half, sin_half, gain_ref, bq_ref, bk_ref, bv_ref, cos_ref, sin_ref, wbuf, kv, kst, qbuf, qst, run_max, run_sum, mixed, obuf, ost, summed,
    xsem, smallsem, wkvsem, wqsem, wosem, ysem, csem,
    kv_recv, kv_send, q_recv, q_send, o_recv, o_send, fwd_send,
):
    me = lax.axis_index("sp")
    chip = lax.div(me, 2)
    core = lax.rem(me, 2)
    other = 1 - core
    up = lax.rem(chip + 1, CHIPS)
    down = lax.rem(chip + CHIPS - 1, CHIPS)
    tokens = xbuf.shape[0]
    block = 2 * tokens
    my_rows = pl.ds(pl.multiple_of(core * tokens, 128), tokens)
    other_rows = pl.ds(pl.multiple_of(other * tokens, 128), tokens)

    def is_chip(n):
        return chip == n

    def device(on_chip, on_core):
        return {"sp": on_chip * 2 + on_core}

    def remote(src, dst, send_sem, recv_sem, on_chip, on_core):
        return pltpu.make_async_remote_copy(
            src_ref=src, dst_ref=dst, send_sem=send_sem, recv_sem=recv_sem,
            device_id=device(on_chip, on_core), device_id_type=pl.DeviceIdType.MESH,
        )

    barrier = pltpu.get_barrier_semaphore()
    for on_chip, on_core in ((chip, other), (up, core), (up, other), (down, core), (down, other)):
        pl.semaphore_signal(barrier, inc=1, device_id=device(on_chip, on_core), device_id_type=pl.DeviceIdType.MESH)

    def group_at(i):
        return jnp.where(i < 2, 1 - i, i)

    def kv_load(i, kind):
        w_hbm = wk_hbm if kind == 0 else wv_hbm
        cols = pl.ds(pl.multiple_of(group_at(i) * 256, 256), 256)
        return pltpu.make_async_copy(
            w_hbm.at[:, cols], wbuf.at[i, :, kind * 256 : (kind + 1) * 256], wkvsem.at[i, kind])

    def wide_load(w_hbm, g, sem):
        cols = pl.ds(pl.multiple_of(g * 768, 256), 768)
        return pltpu.make_async_copy(w_hbm.at[:, cols], wbuf.at[g], sem.at[g])

    def x_copy(n):
        rows = pl.ds(n * (tokens // 4), tokens // 4)
        return pltpu.make_async_copy(x_hbm.at[rows], xbuf.at[rows], xsem.at[n])

    small_copies = [
        pltpu.make_async_copy(src, dst, smallsem.at[n])
        for n, (src, dst) in enumerate((
            (gain_hbm, gain_ref), (bk_hbm, bk_ref), (bv_hbm, bv_ref), (bq_hbm, bq_ref), (cos_hbm, cos_half), (sin_hbm, sin_half)))
    ]
    x_copy(0).start()
    small_copies[0].start()
    for n in range(1, 4):
        x_copy(n).start()
    for copy in small_copies[1:]:
        copy.start()
    small_copies[0].wait()
    gain = gain_ref[...].astype(F32)[None]
    for n in range(4):
        with jax.named_scope("x_wait"):
            x_copy(n).wait()
        if n == 1:
            for i in range(GROUPS):
                for kind in range(2):
                    kv_load(jnp.int32(i), kind).start()
        for start in range(n * (tokens // 4), (n + 1) * (tokens // 4), 32):
            wide = xbuf[start : start + 32, :].astype(F32)
            inv_rms = lax.rsqrt(jnp.mean(wide * wide, axis=-1, keepdims=True) + NORM_EPS)
            hbuf[start : start + 32, :] = (wide * inv_rms * gain).astype(BF16)

    for copy in small_copies[1:]:
        copy.wait()
    cos_ref[...] = jnp.concatenate([cos_half[...], cos_half[...]], axis=1)
    sin_ref[...] = jnp.concatenate([-sin_half[...], sin_half[...]], axis=1)
    with jax.named_scope("entry"):
        pl.semaphore_wait(barrier, 5)

    def rope(u):
        wide = u.astype(F32)
        return (wide * cos_ref[...] + pltpu.roll(wide, HEAD_DIM // 2, 1) * sin_ref[...]).astype(BF16)

    def goes_partner(g):
        return jnp.logical_not((chip == 3) & (g == 0))

    def goes_up(g):
        return (chip <= 1) | ((chip == 2) & (g >= 1)) | ((chip == 3) & (g == 0))

    def goes_down(g):
        return ((chip == 0) & (g >= 1)) | ((chip == 1) & ((g == 0) | (g == 3))) | ((chip == 2) & ((g == 0) | (g == 2))) | ((chip == 3) & (g == 2))

    def own_pair(g, first, on_chip):
        dst = kv.at[chip, g, :, my_rows, :]
        recv = kv_recv.at[chip, g, core]
        return [
            remote(dst, dst, kv_send.at[g, first], recv, on_chip, core),
            remote(kst.at[g], dst, kv_send.at[g, first + 1], recv, on_chip, other)]

    def own_copies(g):
        dst = kv.at[chip, g, :, my_rows, :]
        yield goes_partner(g), [remote(kst.at[g], dst, kv_send.at[g, 0], kv_recv.at[chip, g, core], chip, other)]
        yield goes_up(g), own_pair(g, 1, up)
        yield goes_down(g), own_pair(jnp.where((chip == 2) & (g == 2), 1, g), 3, down)

    def late_copies(g):
        yield (chip == 3) & (g == 1), own_pair(g, 1, up)

    def each(copies, act):
        for go, group in copies:
            @pl.when(go)
            def _():
                for copy in group:
                    act(copy)

    @pl.loop(0, GROUPS)
    def _(i):
        g = group_at(i)
        cols = pl.ds(pl.multiple_of(g * 256, 256), 256)
        for kind in range(2):
            kv_load(i, kind).wait()
        with jax.named_scope("kv_proj"):
            for kind, b_ref in ((0, bk_ref), (1, bv_ref)):
                u = (matmul(hbuf[...], wbuf[i, :, kind * 256 : (kind + 1) * 256]) + b_ref[cols].astype(F32)[None]).astype(BF16)
                even, odd = lane_blocks(u)
                if kind == 0:
                    even, odd = rope(even), rope(odd)
                kv[chip, g, kind, my_rows, :] = jnp.where(core == 0, even, odd)
                kst[g, kind] = jnp.where(core == 0, odd, even)

        wide_load(wq_hbm, i, wqsem).start()
        each(own_copies(g), lambda copy: copy.start())

    def wait_straight(s, g):
        for j in range(2):
            part = kv.at[s, g, :, pl.ds(j * tokens, tokens), :]
            pltpu.make_async_copy(part, part, kv_recv.at[s, g, j]).wait()

    def wait_passed(s, g):
        pltpu.make_async_copy(kv.at[s, g], kv.at[s, g], kv_recv.at[s, g, 0]).wait()

    def pass_on(s, g, to_chip, slot):
        return remote(kv.at[s, g], kv.at[s, g], fwd_send.at[slot], kv_recv.at[s, g, 0], to_chip, core)

    def q_copies(g):
        mine = qbuf.at[g, :, my_rows, :]
        away = (chip == 3) & (g == 0)
        yield jnp.logical_not(away), [
            remote(qst.at[g], mine, q_send.at[g, 0], q_recv.at[g, core], chip, other)]
        there = qbuf.at[GROUPS, :, my_rows, :]
        yield away, [
            remote(mine, there, q_send.at[g, 1], q_recv.at[GROUPS, core], up, core),
            remote(qst.at[g], there, q_send.at[g, 0], q_recv.at[GROUPS, core], up, other)]

    @pl.loop(0, GROUPS)
    def _(g):
        @pl.when(g == GROUPS - 1)
        def _():
            @pl.when(chip == 1)
            def _():
                wait_straight(2, 0)
                pass_on(2, 0, 0, 1).start()

            @pl.when(chip == 2)
            def _():
                wait_straight(1, 1)
                pass_on(1, 1, 3, 0).start()

            @pl.when(chip == 3)
            def _():
                wait_straight(0, 1)
                pass_on(0, 1, 2, 0).start()

        with jax.named_scope("q_wait"):
            wide_load(wq_hbm, g, wqsem).wait()
        with jax.named_scope("q_proj"):
            heads = []
            for n in range(3):
                cols = pl.ds(pl.multiple_of(g * 768 + n * 256, 256), 256)
                u = (matmul_halves(hbuf, wbuf[g, :, n * 256 : (n + 1) * 256]) + bq_ref[cols].astype(F32)[None]).astype(BF16)
                heads += [rope(part) for part in lane_blocks(u)]
            for r in range(REPS):
                even, odd = heads[r], heads[REPS + r]
                qbuf[g, r, my_rows, :] = jnp.where(core == 0, even, odd)
                qst[g, r] = jnp.where(core == 0, odd, even)
        wide_load(wo_hbm, g, wosem).start()
        each(q_copies(g), lambda copy: copy.start())
        each(late_copies(g), lambda copy: copy.start())

    q_tiles = block // TILE

    def tile_rows(t):
        return t // q_tiles, slice((t % q_tiles) * TILE, (t % q_tiles + 1) * TILE)

    def masked_item(q_slot, slot, s, g):
        def score(t):
            r, rows = tile_rows(t)
            sc = matmul_t(qbuf[q_slot, r, rows, :], kv[s, g, 0, 0 : rows.stop, :])
            seen = lax.broadcasted_iota(jnp.int32, (TILE, TILE), 0) >= lax.broadcasted_iota(jnp.int32, (TILE, TILE), 1)
            last = jnp.where(seen, sc[:, rows.start :], -jnp.inf)
            return last if rows.start == 0 else jnp.concatenate([sc[:, : rows.start], last], axis=1)

        def soft(t, sc):
            r, rows = tile_rows(t)
            parts = lane_blocks(sc)
            top = functools.reduce(jnp.maximum, parts)
            top = jnp.broadcast_to(jnp.max(top, axis=1, keepdims=True) * SCORE_SCALE, (TILE, 128))
            probs = [jnp.exp2(part * SCORE_SCALE - top) for part in parts]
            run_max[slot, r, rows, :] = top
            run_sum[slot, r, rows, :] = functools.reduce(jnp.add, probs)
            return (jnp.concatenate([p.astype(BF16) for p in probs], axis=1),)

        def mix(t, probs):
            r, rows = tile_rows(t)
            mixed[slot, r, rows, :] = matmul(probs, kv[s, g, 1, 0 : rows.stop, :])

        pipelined(REPS * q_tiles, score, soft, mix)

    def full_item(q_slot, slot, s, g):
        def score(t):
            r, rows = tile_rows(t)
            return matmul_t(qbuf[q_slot, r, rows, :], kv[s, g, 0])

        def soft(t, sc):
            r, rows = tile_rows(t)
            parts = lane_blocks(sc)
            before = run_max[slot, r, rows, :]
            top = functools.reduce(jnp.maximum, parts)
            top = jnp.maximum(before, jnp.max(top, axis=1, keepdims=True) * SCORE_SCALE)
            rescale = jnp.exp2(before - top)
            probs = [jnp.exp2(part * SCORE_SCALE - top) for part in parts]
            run_max[slot, r, rows, :] = top
            run_sum[slot, r, rows, :] = run_sum[slot, r, rows, :] * rescale + functools.reduce(jnp.add, probs)
            return jnp.concatenate([p.astype(BF16) for p in probs], axis=1), rescale

        def mix(t, probs, rescale):
            r, rows = tile_rows(t)
            mixed[slot, r, rows, :] = mixed[slot, r, rows, :] * rescale + matmul(probs, kv[s, g, 1])

        pipelined(REPS * q_tiles, score, soft, mix)

    def head_cols(g, parity):
        return pl.ds(pl.multiple_of((2 * g + parity) * REPS * 128, 128), REPS * 128)

    def normalized(slot, r, rows):
        total = jnp.sum(run_sum[slot, r, rows, :], axis=1, keepdims=True)
        return (mixed[slot, r, rows, :] / total).astype(BF16)

    def o_copy(g):
        return remote(ost.at[g], obuf.at[:, head_cols(g, core)], o_send.at[g], o_recv.at[g, core], chip, other)

    def finish(g):
        for r in range(REPS):
            ost[g, :, r * 128 : (r + 1) * 128] = normalized(g, r, other_rows)
        o_copy(g).start()
        for r in range(REPS):
            cols = pl.ds(pl.multiple_of(((2 * g + core) * REPS + r) * 128, 128), 128)
            obuf[:, cols] = normalized(g, r, my_rows)

    def back_copies():
        for j in range(2):
            yield remote(ost.at[GROUPS + j], obuf.at[:, head_cols(0, core)], o_send.at[GROUPS + j], o_recv.at[0, core], down, j)

    low = jnp.where(chip == 3, 1, 0)

    @pl.loop(low, jnp.where(chip == 0, GROUPS + 1, GROUPS))
    def _(i):
        g = lax.rem(i, GROUPS)

        @pl.when(i < GROUPS)
        def _():
            part = qbuf.at[i, :, other_rows, :]
            pltpu.make_async_copy(part, part, q_recv.at[i, other]).wait()
            part = kv.at[chip, g, :, other_rows, :]
            pltpu.make_async_copy(part, part, kv_recv.at[chip, g, other]).wait()

        @pl.when(i == GROUPS)
        def _():
            wait_straight(1, 3)
            pass_on(1, 3, 3, 0).start()
            wait_straight(3, 0)
            for j in range(2):
                part = qbuf.at[GROUPS, :, pl.ds(j * tokens, tokens), :]
                pltpu.make_async_copy(part, part, q_recv.at[GROUPS, j]).wait()

        with jax.named_scope('masked'):
            masked_item(i, g, jnp.where(i == GROUPS, 3, chip), g)

        @pl.when((chip == 0) & (i < GROUPS))
        def _():
            finish(i)

    def wait_o(g, parity):
        part = obuf.at[:, head_cols(g, parity)]
        pltpu.make_async_copy(part, part, o_recv.at[g, parity]).wait()

    def out_parts(n):
        for part in range(3):
            yield part, pl.ds(pl.multiple_of(n * 768 + part * 256, 256), 256)

    def out_product(n, part, g):
        weight = wbuf[n, g * 768 : (g + 1) * 768, part * 256 : (part + 1) * 256]
        return matmul_halves(obuf.at[:, g * 768 : (g + 1) * 768], weight)

    tables = (
        ((0, 1, 2, 4), (0, 0, 0, 0)),
        ((0, 0, 0, 0, 4), (1, 0, 2, 3, 0)),
        ((1, 1, 0, 1, 0, 1, 0, 4, 0), (1, 0, 1, 2, 2, 3, 3, 0, 0)),
        ((0, 2, 0, 0, 2, 2, 1, 1, 4, 1), (2, 1, 1, 3, 2, 3, 1, 3, 0, 2)),
    )

    @pl.loop(0, pick(chip, [len(sources) for sources, _ in tables]))
    def _(i):
        s = pick(chip, [pick(i, sources) for sources, _ in tables])
        g = pick(chip, [pick(i, groups) for _, groups in tables])
        @pl.when(s < CHIPS)
        def _():
            q_slot = jnp.where(chip == 0, GROUPS, g)
            is_passed = ((chip == 0) & (s == 2)) | ((chip == 2) & (s == 0)) | ((chip == 3) & (s == 1))
            is_here = ((chip == 0) & (s == 0)) | ((chip == 2) & (s == 1) & (g == 1)) | ((chip == 3) & (s == 0) & (g == 1))

            with jax.named_scope("item_wait"):
                @pl.when(is_passed)
                def _():
                    wait_passed(s, g)

                @pl.when(jnp.logical_not(is_passed | is_here))
                def _():
                    wait_straight(s, g)

            @pl.when((chip == 0) & (s == 2))
            def _():
                wait_straight(3, 1)
                pass_on(3, 1, 1, 1).start()

            @pl.when((chip == 1) & (g == 0))
            def _():
                pass_on(0, 0, 2, 0).start()

            @pl.when((chip == 2) & (s == 1) & (g == 2))
            def _():
                pass_on(1, 2, 3, 1).start()

            @pl.when((chip == 3) & (s == 0) & (g >= 2))
            def _():
                pass_on(0, g, 2, g - 1).start()

            with jax.named_scope('full'):
                full_item(q_slot, g, s, g)

            @pl.when((chip == 1) | ((chip == 2) & (s == 0)) | ((chip == 3) & (s == 1)))
            def _():
                finish(g)

            @pl.when((chip == 0) & (s == 2))
            def _():
                for j in range(2):
                    rows = pl.ds(j * tokens, tokens)
                    for r in range(REPS):
                        ost[GROUPS + j, :, r * 128 : (r + 1) * 128] = normalized(0, r, rows)
                for copy in back_copies():
                    copy.start()

        @pl.when(s == CHIPS)
        def _():
            wait_o(1, other)
            wait_o(3, other)

            @pl.loop(0, 4)
            def _(n):
                wide_load(wo_hbm, n, wosem).wait()
                with jax.named_scope("o_proj_a"):
                    for part, cols in out_parts(n):
                        summed[:, cols] = xbuf[:, cols].astype(F32) + (out_product(n, part, 1) + out_product(n, part, 3))

    @pl.when(chip == 1)
    def _():
        wait_straight(2, 1)
        wait_passed(3, 1)

    @pl.when(chip == 2)
    def _():
        wait_straight(3, 2)

    cache_copies = []
    for s in range(CHIPS):
        for kind, c_hbm in ((0, kc_hbm), (1, vc_hbm)):
            cache_copies.append(
                pltpu.make_async_copy(kv.at[s, chip, kind], c_hbm.at[pl.ds(s * block, block), :], csem.at[s, kind]))
    for copy in cache_copies:
        copy.start()

    with jax.named_scope("o_wait"):
        wait_o(2, other)

        @pl.when(chip < 3)
        def _():
            wait_o(0, other)

        @pl.when(chip == 3)
        def _():
            for parity in range(2):
                wait_o(0, parity)

    def y_copy(n):
        cols = pl.ds(pl.multiple_of(n * 768, 256), 768)
        return pltpu.make_async_copy(xbuf.at[:, cols], y_hbm.at[:, cols], ysem.at[n])

    @pl.loop(0, 4)
    def _(n):
        with jax.named_scope("o_proj"):
            for part, cols in out_parts(n):
                xbuf[:, cols] = (summed[:, cols] + (out_product(n, part, 0) + out_product(n, part, 2))).astype(BF16)
        y_copy(n).start()

    @pl.loop(0, GROUPS)
    def _(g):
        each(own_copies(g), lambda copy: copy.wait_send())
        each(q_copies(g), lambda copy: copy.wait_send())
        each(late_copies(g), lambda copy: copy.wait_send())

    @pl.loop(low, GROUPS)
    def _(g):
        o_copy(g).wait_send()

    @pl.when(chip == 0)
    def _():
        for copy in back_copies():
            copy.wait_send()

    for slot in range(2):
        pass_on(0, 0, up, slot).wait_send()

    @pl.when(chip == 3)
    def _():
        pass_on(0, 0, up, 2).wait_send()

    for copy in cache_copies:
        copy.wait()

    @pl.loop(0, 4)
    def _(n):
        y_copy(n).wait()


def hand_over(*refs):
    count = len(refs) // 3
    sources, targets, buffers = refs[:count], refs[count : 2 * count], refs[2 * count : 3 * count]
    in_sem, out_sem = refs[3 * count :]
    pieces = []
    for n in range(count):
        rows = sources[n].shape[0] // 4
        for part in range(4):
            at = pl.ds(part * rows, rows)
            slot = len(pieces)
            pieces.append((
                pltpu.make_async_copy(sources[n].at[at], buffers[n].at[at], in_sem.at[slot]),
                pltpu.make_async_copy(buffers[n].at[at], targets[n].at[at], out_sem.at[slot])))
    for load, _ in pieces:
        load.start()
    for load, store in pieces:
        load.wait()
        store.start()
    for _, store in pieces:
        store.wait()


def solution(mesh):
    group_size = mesh.shape['sp']
    row_spec = P(('dp', 'sp'), None)
    pos_spec = P(('dp', 'sp'))
    cache_spec = P('dp', 'sp', None)
    whole = P()

    def local(hidden, positions, norm_gain, w_q, b_q, w_k, b_k, w_v, b_v, w_o):
        tokens, width = hidden.shape
        block = 2 * tokens
        seq_len = tokens * group_size
        cosine, sine = rope_tables(positions)
        small = (norm_gain, b_q, b_k, b_v)
        anywhere = pl.BlockSpec(memory_space=pl.ANY)
        dma = pltpu.SemaphoreType.DMA
        y, keys, values = pl.pallas_call(
            kernel,
            out_shape=[
                jax.ShapeDtypeStruct((tokens, width), BF16),
                jax.ShapeDtypeStruct((seq_len, HEAD_DIM), BF16),
                jax.ShapeDtypeStruct((seq_len, HEAD_DIM), BF16),
            ],
            in_specs=[anywhere] * 11,
            out_specs=[anywhere] * 3,
            scratch_shapes=[
                pltpu.VMEM((tokens, width), BF16),
                pltpu.VMEM((tokens, width), BF16),
                pltpu.VMEM((tokens, HEAD_DIM // 2), F32),
                pltpu.VMEM((tokens, HEAD_DIM // 2), F32),
                *(pltpu.VMEM(a.shape, BF16) for a in small),
                pltpu.VMEM((tokens, HEAD_DIM), F32),
                pltpu.VMEM((tokens, HEAD_DIM), F32),
                pltpu.VMEM((GROUPS, width, 768), BF16),
                pltpu.VMEM((CHIPS, GROUPS, 2, block, HEAD_DIM), BF16),
                pltpu.VMEM((GROUPS, 2, tokens, HEAD_DIM), BF16),
                pltpu.VMEM((GROUPS + 1, REPS, block, HEAD_DIM), BF16),
                pltpu.VMEM((GROUPS, REPS, tokens, HEAD_DIM), BF16),
                pltpu.VMEM((GROUPS, REPS, block, HEAD_DIM), F32),
                pltpu.VMEM((GROUPS, REPS, block, HEAD_DIM), F32),
                pltpu.VMEM((GROUPS, REPS, block, HEAD_DIM), F32),
                pltpu.VMEM((tokens, width), BF16),
                pltpu.VMEM((GROUPS + 2, tokens, REPS * HEAD_DIM), BF16),
                pltpu.VMEM((tokens, width), F32),
                dma((4,)), dma((6,)), dma((GROUPS, 2)), dma((4,)), dma((4,)), dma((4,)), dma((CHIPS, 2)),
                dma((CHIPS, GROUPS, 2)), dma((GROUPS, 5)), dma((GROUPS + 1, 2)), dma((GROUPS, 2)),
                dma((GROUPS, 2)), dma((GROUPS + 2,)), dma((3,)),
            ],
            compiler_params=pltpu.CompilerParams(
                collective_id=0, has_side_effects=True, vmem_limit_bytes=67043328),
            name="block",
        )(
            hidden, cosine, sine, *small, w_q, w_k, w_v, w_o,
        )
        results = (y, keys, values)
        y, keys, values = pl.pallas_call(
            hand_over,
            out_shape=[jax.ShapeDtypeStruct(a.shape, a.dtype) for a in results],
            in_specs=[anywhere] * 3,
            out_specs=[anywhere] * 3,
            scratch_shapes=[pltpu.VMEM(a.shape, a.dtype) for a in results] + [dma((12,)), dma((12,))],
            name="hand_over",
        )(*results)
        return y, keys[:, None, :], values[:, None, :]

    return jax.shard_map(local, mesh=mesh, in_specs=(row_spec, pos_spec, whole, whole, whole, whole, whole, whole, whole, whole), out_specs=(row_spec, cache_spec, cache_spec), check_vma=False)
```

```python
import functools
import math

import jax
import jax.numpy as jnp
from jax import lax
from jax.experimental import pallas as pl
from jax.experimental.pallas import tpu as pltpu
from jax.sharding import PartitionSpec as P

HEAD_DIM = 128
ROPE_BASE = 1000000.0
NORM_EPS = 1e-6
SCORE_SCALE = math.log2(math.e) / math.sqrt(HEAD_DIM)
CHIPS = 4
GROUPS = 4
REPS = 3
TILE = 256
BF16 = jnp.bfloat16
F32 = jnp.float32


def rope_tables(positions):
    half_dim = HEAD_DIM // 2
    inv_freq = ROPE_BASE ** (-2.0 * jnp.arange(half_dim, dtype=F32) / HEAD_DIM)
    angle = positions.astype(F32) * inv_freq[:, None]
    return jnp.cos(angle), jnp.sin(angle)


def matmul(a, b):
    return lax.dot_general(a, b, (((1,), (0,)), ((), ())), preferred_element_type=F32)


def matmul_t(a, b):
    return lax.dot_general(a, b, (((1,), (1,)), ((), ())), preferred_element_type=F32)


def matmul_tn(a, b):
    return lax.dot_general(a, b, (((0,), (0,)), ((), ())), preferred_element_type=F32)


def matmul_halves(a_ref, b):
    half = a_ref.shape[0] // 2
    return jnp.concatenate([matmul(a_ref[:half], b), matmul(a_ref[half:], b)], axis=0)


def pick(i, values):
    out = values[-1]
    for n in range(len(values) - 1):
        out = jnp.where(i == n, values[n], out)
    return out


def lane_blocks(x):
    return [x[:, i : i + 128] for i in range(0, x.shape[1], 128)]


def row_blocks(x):
    return [x[i : i + 8] for i in range(0, x.shape[0], 8)]


def pipelined(count, score, soft, mix):
    scores, weights = {}, {}
    for t in range(count + 2):
        if t < count:
            scores[t] = score(t)
        if 0 <= t - 1 < count:
            weights[t - 1] = soft(t - 1, scores.pop(t - 1))
        if 0 <= t - 2 < count:
            mix(t - 2, *weights.pop(t - 2))


def kernel(
    x_hbm, cos_hbm, sin_hbm, gain_hbm, bq_hbm, bk_hbm, bv_hbm, wq_hbm, wk_hbm, wv_hbm, wo_hbm,
    y_hbm, kc_hbm, vc_hbm,
    xbuf, hbuf, cos_half, sin_half, gain_ref, bq_ref, bk_ref, bv_ref, cos_ref, sin_ref, wbuf, kv, kst, qbuf, qst, run_max, run_sum, mixed, obuf, ost, summed,
    xsem, smallsem, wkvsem, wqsem, wosem, ysem, csem,
    kv_recv, kv_send, q_recv, q_send, o_recv, o_send, fwd_send,
):
    me = lax.axis_index("sp")
    chip = lax.div(me, 2)
    core = lax.rem(me, 2)
    other = 1 - core
    up = lax.rem(chip + 1, CHIPS)
    down = lax.rem(chip + CHIPS - 1, CHIPS)
    tokens = xbuf.shape[0]
    block = 2 * tokens
    my_rows = pl.ds(pl.multiple_of(core * tokens, 128), tokens)
    other_rows = pl.ds(pl.multiple_of(other * tokens, 128), tokens)

    def is_chip(n):
        return chip == n

    def device(on_chip, on_core):
        return {"sp": on_chip * 2 + on_core}

    def remote(src, dst, send_sem, recv_sem, on_chip, on_core):
        return pltpu.make_async_remote_copy(
            src_ref=src, dst_ref=dst, send_sem=send_sem, recv_sem=recv_sem,
            device_id=device(on_chip, on_core), device_id_type=pl.DeviceIdType.MESH,
        )

    barrier = pltpu.get_barrier_semaphore()
    for on_chip, on_core in ((chip, other), (up, core), (up, other), (down, core), (down, other)):
        pl.semaphore_signal(barrier, inc=1, device_id=device(on_chip, on_core), device_id_type=pl.DeviceIdType.MESH)

    def group_at(i):
        return jnp.where((chip < 3) & (i < 2), 1 - i, i)

    def kv_load(i, kind):
        w_hbm = wk_hbm if kind == 0 else wv_hbm
        cols = pl.ds(pl.multiple_of(group_at(i) * 256, 256), 256)
        return pltpu.make_async_copy(
            w_hbm.at[:, cols], wbuf.at[i, :, kind * 256 : (kind + 1) * 256], wkvsem.at[i, kind])

    def wide_load(w_hbm, g, sem):
        cols = pl.ds(pl.multiple_of(g * 768, 256), 768)
        return pltpu.make_async_copy(w_hbm.at[:, cols], wbuf.at[g], sem.at[g])

    def x_copy(n):
        rows = pl.ds(n * (tokens // 4), tokens // 4)
        return pltpu.make_async_copy(x_hbm.at[rows], xbuf.at[rows], xsem.at[n])

    small_copies = [
        pltpu.make_async_copy(src, dst, smallsem.at[n])
        for n, (src, dst) in enumerate((
            (gain_hbm, gain_ref), (bk_hbm, bk_ref), (bv_hbm, bv_ref), (bq_hbm, bq_ref), (cos_hbm, cos_half), (sin_hbm, sin_half)))
    ]
    x_copy(0).start()
    small_copies[0].start()
    x_copy(1).start()
    for kind in range(2):
        kv_load(jnp.int32(0), kind).start()
    for n in range(2, 4):
        x_copy(n).start()
    for copy in small_copies[1:]:
        copy.start()
    small_copies[0].wait()
    gain = gain_ref[...].astype(F32)[None]
    for n in range(4):
        with jax.named_scope("x_wait"):
            x_copy(n).wait()
        if n == 1:
            for i in range(1, GROUPS):
                for kind in range(2):
                    kv_load(jnp.int32(i), kind).start()
        for start in range(n * (tokens // 4), (n + 1) * (tokens // 4), 32):
            wide = xbuf[start : start + 32, :].astype(F32)
            inv_rms = lax.rsqrt(jnp.mean(wide * wide, axis=-1, keepdims=True) + NORM_EPS)
            hbuf[start : start + 32, :] = (wide * inv_rms * gain).astype(BF16)

    for copy in small_copies[1:]:
        copy.wait()
    cos_ref[...] = jnp.transpose(jnp.concatenate([cos_half[...], cos_half[...]], axis=0))
    sin_ref[...] = jnp.transpose(jnp.concatenate([-sin_half[...], sin_half[...]], axis=0))
    with jax.named_scope("entry"):
        pl.semaphore_wait(barrier, 5)

    def rope(u):
        wide = u.astype(F32)
        return (wide * cos_ref[...] + pltpu.roll(wide, HEAD_DIM // 2, 1) * sin_ref[...]).astype(BF16)

    def goes_partner(g):
        return jnp.logical_not((chip == 3) & (g == 0))

    def goes_up(g):
        return (chip <= 1) | ((chip == 2) & ((g == 1) | (g == 2))) | ((chip == 3) & (g == 0))

    def goes_down(g):
        return ((chip == 0) & (g >= 1)) | ((chip == 1) & ((g == 0) | (g == 3))) | ((chip == 2) & ((g == 0) | (g == 2))) | ((chip == 3) & (g == 2))

    def own_pair(g, first, on_chip):
        dst = kv.at[chip, g, :, my_rows, :]
        recv = kv_recv.at[chip, g, core]
        return [
            remote(dst, dst, kv_send.at[g, first], recv, on_chip, core),
            remote(kst.at[g], dst, kv_send.at[g, first + 1], recv, on_chip, other)]

    def own_copies(g):
        dst = kv.at[chip, g, :, my_rows, :]
        yield goes_partner(g), [remote(kst.at[g], dst, kv_send.at[g, 0], kv_recv.at[chip, g, core], chip, other)]
        yield goes_up(g), own_pair(g, 1, up)
        yield goes_down(g), own_pair(jnp.where((chip == 2) & (g == 2), 1, g), 3, down)

    def late_pair():
        return own_pair(jnp.where(chip == 2, 3, 1), 1, up)

    def each(copies, act):
        for go, group in copies:
            @pl.when(go)
            def _():
                for copy in group:
                    act(copy)

    @pl.loop(0, GROUPS)
    def _(i):
        g = group_at(i)
        cols = pl.ds(pl.multiple_of(g * 256, 256), 256)
        for kind in range(2):
            kv_load(i, kind).wait()
        with jax.named_scope("kv_proj"):
            for kind, b_ref in ((0, bk_ref), (1, bv_ref)):
                u = (matmul(hbuf[...], wbuf[i, :, kind * 256 : (kind + 1) * 256]) + b_ref[cols].astype(F32)[None]).astype(BF16)
                even, odd = lane_blocks(u)
                if kind == 0:
                    even, odd = rope(even), rope(odd)
                kv[chip, g, kind, my_rows, :] = jnp.where(core == 0, even, odd)
                kst[g, kind] = jnp.where(core == 0, odd, even)

        wide_load(wq_hbm, i, wqsem).start()
        each(own_copies(g), lambda copy: copy.start())

    def wait_straight(s, g):
        for j in range(2):
            part = kv.at[s, g, :, pl.ds(j * tokens, tokens), :]
            pltpu.make_async_copy(part, part, kv_recv.at[s, g, j]).wait()

    def wait_passed(s, g):
        pltpu.make_async_copy(kv.at[s, g], kv.at[s, g], kv_recv.at[s, g, 0]).wait()

    def pass_on(s, g, to_chip, slot):
        return remote(kv.at[s, g], kv.at[s, g], fwd_send.at[slot], kv_recv.at[s, g, 0], to_chip, core)

    def q_copies(g):
        mine = qbuf.at[g, :, my_rows, :]
        away = (chip == 3) & (g == 0)
        yield jnp.logical_not(away), [
            remote(qst.at[g], mine, q_send.at[g, 0], q_recv.at[g, core], chip, other)]
        there = qbuf.at[GROUPS, :, my_rows, :]
        yield away, [
            remote(mine, there, q_send.at[g, 1], q_recv.at[GROUPS, core], up, core),
            remote(qst.at[g], there, q_send.at[g, 0], q_recv.at[GROUPS, core], up, other)]

    @pl.loop(0, GROUPS)
    def _(g):
        @pl.when(g == GROUPS - 1)
        def _():
            @pl.when(chip == 1)
            def _():
                wait_straight(2, 0)
                pass_on(2, 0, 0, 1).start()

            @pl.when(chip == 2)
            def _():
                wait_straight(1, 1)
                pass_on(1, 1, 3, 0).start()
                for copy in late_pair():
                    copy.start()

            @pl.when(chip == 3)
            def _():
                wait_straight(0, 1)
                pass_on(0, 1, 2, 0).start()

        with jax.named_scope("q_wait"):
            wide_load(wq_hbm, g, wqsem).wait()
        with jax.named_scope("q_proj"):
            heads = []
            for n in range(3):
                cols = pl.ds(pl.multiple_of(g * 768 + n * 256, 256), 256)
                u = (matmul_halves(hbuf, wbuf[g, :, n * 256 : (n + 1) * 256]) + bq_ref[cols].astype(F32)[None]).astype(BF16)
                heads += [rope(part) for part in lane_blocks(u)]
            for r in range(REPS):
                even, odd = heads[r], heads[REPS + r]
                qbuf[g, r, my_rows, :] = jnp.where(core == 0, even, odd)
                qst[g, r] = jnp.where(core == 0, odd, even)
        wide_load(wo_hbm, g, wosem).start()
        each(q_copies(g), lambda copy: copy.start())

    def masked_item(q_slot, slot, s, g):
        tiles = [(r, slice(start, start + TILE)) for r in range(REPS) for start in range(0, block, TILE)]

        def score(t):
            r, at = tiles[t]
            sc = matmul_t(kv[s, g, 0, 0 : at.stop, :], qbuf[q_slot, r, at, :])
            seen = lax.broadcasted_iota(jnp.int32, (TILE, TILE), 0) <= lax.broadcasted_iota(jnp.int32, (TILE, TILE), 1)
            last = jnp.where(seen, sc[at.start :], -jnp.inf)
            return last if at.start == 0 else jnp.concatenate([sc[: at.start], last], axis=0)

        def soft(t, sc):
            r, at = tiles[t]
            parts = row_blocks(sc)
            top = jnp.max(functools.reduce(jnp.maximum, parts), axis=0, keepdims=True) * SCORE_SCALE
            top = jnp.broadcast_to(top, (8, TILE))
            probs = [jnp.exp2(part * SCORE_SCALE - top) for part in parts]
            run_max[slot, r, :, at] = top
            run_sum[slot, r, :, at] = functools.reduce(jnp.add, probs)
            return (jnp.concatenate(probs, axis=0).astype(BF16),)

        def mix(t, probs):
            r, at = tiles[t]
            mixed[slot, r, :, at] = matmul_tn(kv[s, g, 1, 0 : at.stop, :], probs)

        pipelined(len(tiles), score, soft, mix)

    def full_item(q_slot, slot, s, g):
        def score(r):
            return matmul_t(kv[s, g, 0], qbuf[q_slot, r])

        def soft(r, sc):
            parts = row_blocks(sc)
            before = run_max[slot, r]
            top = jnp.max(functools.reduce(jnp.maximum, parts), axis=0, keepdims=True) * SCORE_SCALE
            top = jnp.maximum(before, top)
            rescale = jnp.exp2(before - top)
            probs = [jnp.exp2(part * SCORE_SCALE - top) for part in parts]
            run_max[slot, r] = top
            run_sum[slot, r] = run_sum[slot, r] * rescale + functools.reduce(jnp.add, probs)
            return jnp.concatenate(probs, axis=0).astype(BF16), rescale

        def mix(r, probs, rescale):
            mixed[slot, r] = mixed[slot, r] * rescale[0:1] + matmul_tn(kv[s, g, 1], probs)

        pipelined(REPS, score, soft, mix)

    def head_cols(g, parity):
        return pl.ds(pl.multiple_of((2 * g + parity) * REPS * 128, 128), REPS * 128)

    def normalized(slot, r, rows):
        total = jnp.sum(run_sum[slot, r, :, rows], axis=0, keepdims=True)
        return jnp.transpose(mixed[slot, r, :, rows] / total).astype(BF16)

    def o_copy(g):
        return remote(ost.at[g], obuf.at[:, head_cols(g, core)], o_send.at[g], o_recv.at[g, core], chip, other)

    def finish(g):
        for r in range(REPS):
            ost[g, :, r * 128 : (r + 1) * 128] = normalized(g, r, other_rows)
        o_copy(g).start()
        for r in range(REPS):
            cols = pl.ds(pl.multiple_of(((2 * g + core) * REPS + r) * 128, 128), 128)
            obuf[:, cols] = normalized(g, r, my_rows)

    def back_copies():
        for j in range(2):
            yield remote(ost.at[GROUPS + j], obuf.at[:, head_cols(0, core)], o_send.at[GROUPS + j], o_recv.at[0, core], down, j)

    low = jnp.where(chip == 3, 1, 0)

    @pl.loop(low, jnp.where(chip == 0, GROUPS + 1, GROUPS))
    def _(i):
        g = lax.rem(i, GROUPS)

        @pl.when(i < GROUPS)
        def _():
            part = qbuf.at[i, :, other_rows, :]
            pltpu.make_async_copy(part, part, q_recv.at[i, other]).wait()
            part = kv.at[chip, g, :, other_rows, :]
            pltpu.make_async_copy(part, part, kv_recv.at[chip, g, other]).wait()

        @pl.when(i == GROUPS)
        def _():
            wait_straight(1, 3)
            pass_on(1, 3, 3, 0).start()
            wait_straight(3, 0)
            for j in range(2):
                part = qbuf.at[GROUPS, :, pl.ds(j * tokens, tokens), :]
                pltpu.make_async_copy(part, part, q_recv.at[GROUPS, j]).wait()

        with jax.named_scope('masked'):
            masked_item(i, g, jnp.where(i == GROUPS, 3, chip), g)

        @pl.when((chip == 0) & (i < GROUPS))
        def _():
            finish(i)

    def wait_o(g, parity):
        part = obuf.at[:, head_cols(g, parity)]
        pltpu.make_async_copy(part, part, o_recv.at[g, parity]).wait()

    def out_parts(n):
        for part in range(3):
            yield part, pl.ds(pl.multiple_of(n * 768 + part * 256, 256), 256)

    def out_product(n, part, g):
        weight = wbuf[n, g * 768 : (g + 1) * 768, part * 256 : (part + 1) * 256]
        return matmul_halves(obuf.at[:, g * 768 : (g + 1) * 768], weight)

    tables = (
        ((0, 1, 2, 4, 5), (0, 0, 0, 0, 0)),
        ((0, 0, 0, 0, 4, 5), (1, 0, 2, 3, 0, 0)),
        ((1, 1, 0, 1, 0, 4, 1, 0, 5, 0), (1, 0, 1, 2, 2, 0, 3, 3, 0, 0)),
        ((0, 2, 0, 0, 2, 1, 4, 2, 1, 1, 5), (2, 1, 1, 3, 2, 1, 0, 3, 3, 2, 0)),
    )

    @pl.when(chip == 3)
    def _():
        for copy in late_pair():
            copy.start()

    @pl.loop(0, pick(chip, [len(sources) for sources, _ in tables]))
    def _(i):
        s = pick(chip, [pick(i, sources) for sources, _ in tables])
        g = pick(chip, [pick(i, groups) for _, groups in tables])
        @pl.when(s < CHIPS)
        def _():
            q_slot = jnp.where(chip == 0, GROUPS, g)
            is_passed = ((chip == 0) & (s == 2)) | ((chip == 2) & (s == 0)) | ((chip == 3) & (s == 1))
            is_here = ((chip == 0) & (s == 0)) | ((chip == 2) & (s == 1) & (g == 1)) | ((chip == 3) & (s == 0) & (g == 1))

            with jax.named_scope("item_wait"):
                @pl.when(is_passed)
                def _():
                    wait_passed(s, g)

                @pl.when(jnp.logical_not(is_passed | is_here))
                def _():
                    wait_straight(s, g)

            @pl.when((chip == 0) & (s == 2))
            def _():
                wait_straight(3, 1)
                pass_on(3, 1, 1, 1).start()

            @pl.when((chip == 1) & (g == 0))
            def _():
                pass_on(0, 0, 2, 0).start()

            @pl.when((chip == 2) & (s == 1) & (g == 2))
            def _():
                pass_on(1, 2, 3, 1).start()

            @pl.when((chip == 3) & (s == 0) & (g >= 2))
            def _():
                pass_on(0, g, 2, g - 1).start()

            with jax.named_scope('full'):
                full_item(q_slot, g, s, g)

            @pl.when((chip == 1) | ((chip == 2) & (s == 0)) | ((chip == 3) & (s == 1)))
            def _():
                finish(g)

            @pl.when((chip == 0) & (s == 2))
            def _():
                for j in range(2):
                    rows = pl.ds(j * tokens, tokens)
                    for r in range(REPS):
                        ost[GROUPS + j, :, r * 128 : (r + 1) * 128] = normalized(0, r, rows)
                for copy in back_copies():
                    copy.start()

        @pl.when(s == CHIPS)
        def _():
            wait_o(1, other)

            @pl.loop(0, 4)
            def _(n):
                wide_load(wo_hbm, n, wosem).wait()
                with jax.named_scope("o_proj_a"):
                    for part, cols in out_parts(n):
                        summed[:, cols] = xbuf[:, cols].astype(F32) + out_product(n, part, 1)

        @pl.when(s == CHIPS + 1)
        def _():
            wait_o(3, other)

            @pl.loop(0, 4)
            def _(n):
                with jax.named_scope("o_proj_b"):
                    for part, cols in out_parts(n):
                        summed[:, cols] += out_product(n, part, 3)

    @pl.when(chip == 1)
    def _():
        wait_straight(2, 1)
        wait_passed(3, 1)

    @pl.when(chip == 2)
    def _():
        wait_straight(3, 2)

    cache_copies = []
    for s in range(CHIPS):
        for kind, c_hbm in ((0, kc_hbm), (1, vc_hbm)):
            cache_copies.append(
                pltpu.make_async_copy(kv.at[s, chip, kind], c_hbm.at[pl.ds(s * block, block), :], csem.at[s, kind]))
    for copy in cache_copies:
        copy.start()

    with jax.named_scope("o_wait"):
        wait_o(2, other)

        @pl.when(chip < 3)
        def _():
            wait_o(0, other)

        @pl.when(chip == 3)
        def _():
            for parity in range(2):
                wait_o(0, parity)

    def y_copy(n):
        cols = pl.ds(pl.multiple_of(n * 768, 256), 768)
        return pltpu.make_async_copy(xbuf.at[:, cols], y_hbm.at[:, cols], ysem.at[n])

    @pl.loop(0, 4)
    def _(n):
        with jax.named_scope("o_proj"):
            for part, cols in out_parts(n):
                xbuf[:, cols] = (summed[:, cols] + (out_product(n, part, 0) + out_product(n, part, 2))).astype(BF16)
        y_copy(n).start()

    @pl.loop(0, GROUPS)
    def _(g):
        each(own_copies(g), lambda copy: copy.wait_send())
        each(q_copies(g), lambda copy: copy.wait_send())

    @pl.loop(low, GROUPS)
    def _(g):
        o_copy(g).wait_send()

    @pl.when(chip == 0)
    def _():
        for copy in back_copies():
            copy.wait_send()

    @pl.when(chip >= 2)
    def _():
        for copy in late_pair():
            copy.wait_send()

    for slot in range(2):
        pass_on(0, 0, up, slot).wait_send()

    @pl.when(chip == 3)
    def _():
        pass_on(0, 0, up, 2).wait_send()

    for copy in cache_copies:
        copy.wait()

    @pl.loop(0, 4)
    def _(n):
        y_copy(n).wait()


def hand_over(*refs):
    count = len(refs) // 3
    sources, targets, buffers = refs[:count], refs[count : 2 * count], refs[2 * count : 3 * count]
    in_sem, out_sem = refs[3 * count :]
    pieces = []
    for n in range(count):
        rows = sources[n].shape[0] // 4
        for part in range(4):
            at = pl.ds(part * rows, rows)
            slot = len(pieces)
            pieces.append((
                pltpu.make_async_copy(sources[n].at[at], buffers[n].at[at], in_sem.at[slot]),
                pltpu.make_async_copy(buffers[n].at[at], targets[n].at[at], out_sem.at[slot])))
    for load, _ in pieces:
        load.start()
    for load, store in pieces:
        load.wait()
        store.start()
    for _, store in pieces:
        store.wait()


def solution(mesh):
    group_size = mesh.shape['sp']
    row_spec = P(('dp', 'sp'), None)
    pos_spec = P(('dp', 'sp'))
    cache_spec = P('dp', 'sp', None)
    whole = P()

    def local(hidden, positions, norm_gain, w_q, b_q, w_k, b_k, w_v, b_v, w_o):
        tokens, width = hidden.shape
        block = 2 * tokens
        seq_len = tokens * group_size
        cosine, sine = rope_tables(positions)
        small = (norm_gain, b_q, b_k, b_v)
        anywhere = pl.BlockSpec(memory_space=pl.ANY)
        dma = pltpu.SemaphoreType.DMA
        y, keys, values = pl.pallas_call(
            kernel,
            out_shape=[
                jax.ShapeDtypeStruct((tokens, width), BF16),
                jax.ShapeDtypeStruct((seq_len, HEAD_DIM), BF16),
                jax.ShapeDtypeStruct((seq_len, HEAD_DIM), BF16),
            ],
            in_specs=[anywhere] * 11,
            out_specs=[anywhere] * 3,
            scratch_shapes=[
                pltpu.VMEM((tokens, width), BF16),
                pltpu.VMEM((tokens, width), BF16),
                pltpu.VMEM((HEAD_DIM // 2, tokens), F32),
                pltpu.VMEM((HEAD_DIM // 2, tokens), F32),
                *(pltpu.VMEM(a.shape, BF16) for a in small),
                pltpu.VMEM((tokens, HEAD_DIM), F32),
                pltpu.VMEM((tokens, HEAD_DIM), F32),
                pltpu.VMEM((GROUPS, width, 768), BF16),
                pltpu.VMEM((CHIPS, GROUPS, 2, block, HEAD_DIM), BF16),
                pltpu.VMEM((GROUPS, 2, tokens, HEAD_DIM), BF16),
                pltpu.VMEM((GROUPS + 1, REPS, block, HEAD_DIM), BF16),
                pltpu.VMEM((GROUPS, REPS, tokens, HEAD_DIM), BF16),
                pltpu.VMEM((GROUPS, REPS, 8, block), F32),
                pltpu.VMEM((GROUPS, REPS, 8, block), F32),
                pltpu.VMEM((GROUPS, REPS, HEAD_DIM, block), F32),
                pltpu.VMEM((tokens, width), BF16),
                pltpu.VMEM((GROUPS + 2, tokens, REPS * HEAD_DIM), BF16),
                pltpu.VMEM((tokens, width), F32),
                dma((4,)), dma((6,)), dma((GROUPS, 2)), dma((4,)), dma((4,)), dma((4,)), dma((CHIPS, 2)),
                dma((CHIPS, GROUPS, 2)), dma((GROUPS, 5)), dma((GROUPS + 1, 2)), dma((GROUPS, 2)),
                dma((GROUPS, 2)), dma((GROUPS + 2,)), dma((3,)),
            ],
            compiler_params=pltpu.CompilerParams(
                collective_id=0, has_side_effects=True, vmem_limit_bytes=67043328),
            name="block",
        )(
            hidden, cosine, sine, *small, w_q, w_k, w_v, w_o,
        )
        results = (y, keys, values)
        y, keys, values = pl.pallas_call(
            hand_over,
            out_shape=[jax.ShapeDtypeStruct(a.shape, a.dtype) for a in results],
            in_specs=[anywhere] * 3,
            out_specs=[anywhere] * 3,
            scratch_shapes=[pltpu.VMEM(a.shape, a.dtype) for a in results] + [dma((12,)), dma((12,))],
            name="hand_over",
        )(*results)
        return y, keys[:, None, :], values[:, None, :]

    return jax.shard_map(local, mesh=mesh, in_specs=(row_spec, pos_spec, whole, whole, whole, whole, whole, whole, whole, whole), out_specs=(row_spec, cache_spec, cache_spec), check_vma=False)
```

```python
import functools
import math

import jax
import jax.numpy as jnp
from jax import lax
from jax.experimental import pallas as pl
from jax.experimental.pallas import tpu as pltpu
from jax.sharding import PartitionSpec as P

HEAD_DIM = 128
ROPE_BASE = 1000000.0
NORM_EPS = 1e-6
SCORE_SCALE = math.log2(math.e) / math.sqrt(HEAD_DIM)
CHIPS = 4
GROUPS = 4
REPS = 3
TILE = 384
BF16 = jnp.bfloat16
F32 = jnp.float32


def rope_tables(positions):
    half_dim = HEAD_DIM // 2
    inv_freq = ROPE_BASE ** (-2.0 * jnp.arange(half_dim, dtype=F32) / HEAD_DIM)
    angle = positions.astype(F32) * inv_freq[:, None]
    return jnp.cos(angle), jnp.sin(angle)


def matmul(a, b):
    return lax.dot_general(a, b, (((1,), (0,)), ((), ())), preferred_element_type=F32)


def matmul_t(a, b):
    return lax.dot_general(a, b, (((1,), (1,)), ((), ())), preferred_element_type=F32)


def matmul_tn(a, b):
    return lax.dot_general(a, b, (((0,), (0,)), ((), ())), preferred_element_type=F32)


def matmul_halves(a_ref, b):
    half = a_ref.shape[0] // 2
    return jnp.concatenate([matmul(a_ref[:half], b), matmul(a_ref[half:], b)], axis=0)


def matmul_whole(a_ref, b):
    return matmul(a_ref[...], b)


def pick(i, values):
    out = values[-1]
    for n in range(len(values) - 1):
        out = jnp.where(i == n, values[n], out)
    return out


def lane_blocks(x):
    return [x[:, i : i + 128] for i in range(0, x.shape[1], 128)]


def row_blocks(x):
    return [x[i : i + 8] for i in range(0, x.shape[0], 8)]


def pipelined(count, score, soft, mix):
    scores, weights = {}, {}
    for t in range(count + 2):
        if t < count:
            scores[t] = score(t)
        if 0 <= t - 1 < count:
            weights[t - 1] = soft(t - 1, scores.pop(t - 1))
        if 0 <= t - 2 < count:
            mix(t - 2, *weights.pop(t - 2))


def kernel(
    x_hbm, cos_hbm, sin_hbm, gain_hbm, bq_hbm, bk_hbm, bv_hbm, wq_hbm, wk_hbm, wv_hbm, wo_hbm,
    y_ref, kc_ref, vc_ref,
    xbuf, hbuf, cos_half, sin_half, gain_ref, bq_ref, bk_ref, bv_ref, cos_ref, sin_ref, wbuf, kv, kst, qbuf, qst, run_max, run_sum, mixed, obuf, ost, summed,
    xsem, smallsem, wkvsem, wqsem, wosem,
    kv_recv, kv_send, q_recv, q_send, o_recv, o_send, fwd_send,
):
    me = lax.axis_index("sp")
    chip = lax.div(me, 2)
    core = lax.rem(me, 2)
    other = 1 - core
    up = lax.rem(chip + 1, CHIPS)
    down = lax.rem(chip + CHIPS - 1, CHIPS)
    tokens = xbuf.shape[0]
    block = 2 * tokens
    my_rows = pl.ds(pl.multiple_of(core * tokens, 128), tokens)
    other_rows = pl.ds(pl.multiple_of(other * tokens, 128), tokens)

    def is_chip(n):
        return chip == n

    def device(on_chip, on_core):
        return {"sp": on_chip * 2 + on_core}

    def remote(src, dst, send_sem, recv_sem, on_chip, on_core):
        return pltpu.make_async_remote_copy(
            src_ref=src, dst_ref=dst, send_sem=send_sem, recv_sem=recv_sem,
            device_id=device(on_chip, on_core), device_id_type=pl.DeviceIdType.MESH,
        )

    barrier = pltpu.get_barrier_semaphore()
    for on_chip, on_core in ((chip, other), (up, core), (up, other), (down, core), (down, other)):
        pl.semaphore_signal(barrier, inc=1, device_id=device(on_chip, on_core), device_id_type=pl.DeviceIdType.MESH)

    def group_at(i):
        return jnp.where((chip < 3) & (i < 2), 1 - i, i)

    def kv_load(i, kind):
        w_hbm = wk_hbm if kind == 0 else wv_hbm
        cols = pl.ds(pl.multiple_of(group_at(i) * 256, 256), 256)
        return pltpu.make_async_copy(
            w_hbm.at[:, cols], wbuf.at[i, :, kind * 256 : (kind + 1) * 256], wkvsem.at[i, kind])

    def wide_load(w_hbm, g, sem):
        cols = pl.ds(pl.multiple_of(g * 768, 256), 768)
        return pltpu.make_async_copy(w_hbm.at[:, cols], wbuf.at[g], sem.at[g])

    def x_copy(n):
        rows = pl.ds(n * (tokens // 4), tokens // 4)
        return pltpu.make_async_copy(x_hbm.at[rows], xbuf.at[rows], xsem.at[n])

    small_copies = [
        pltpu.make_async_copy(src, dst, smallsem.at[n])
        for n, (src, dst) in enumerate((
            (gain_hbm, gain_ref), (bk_hbm, bk_ref), (bv_hbm, bv_ref), (bq_hbm, bq_ref), (cos_hbm, cos_half), (sin_hbm, sin_half)))
    ]
    x_copy(0).start()
    small_copies[0].start()
    x_copy(1).start()
    for kind in range(2):
        kv_load(jnp.int32(0), kind).start()
    for n in range(2, 4):
        x_copy(n).start()
    for copy in small_copies[1:]:
        copy.start()
    small_copies[0].wait()
    gain = gain_ref[...].astype(F32)[None]
    for n in range(4):
        with jax.named_scope("x_wait"):
            x_copy(n).wait()
        if n == 1:
            for i in range(1, GROUPS):
                for kind in range(2):
                    kv_load(jnp.int32(i), kind).start()
        for start in range(n * (tokens // 4), (n + 1) * (tokens // 4), 16):
            wide = xbuf[start : start + 16, :].astype(F32)
            inv_rms = lax.rsqrt(jnp.mean(wide * wide, axis=-1, keepdims=True) + NORM_EPS)
            hbuf[start : start + 16, :] = (wide * inv_rms * gain).astype(BF16)

    for copy in small_copies[1:]:
        copy.wait()
    cos_ref[...] = jnp.transpose(jnp.concatenate([cos_half[...], cos_half[...]], axis=0))
    sin_ref[...] = jnp.transpose(jnp.concatenate([-sin_half[...], sin_half[...]], axis=0))
    with jax.named_scope("entry"):
        pl.semaphore_wait(barrier, 5)

    def rope(u):
        wide = u.astype(F32)
        return (wide * cos_ref[...] + pltpu.roll(wide, HEAD_DIM // 2, 1) * sin_ref[...]).astype(BF16)

    def goes_partner(g):
        return jnp.logical_not((chip == 3) & (g == 0))

    def goes_up(g):
        return (chip <= 1) | ((chip == 2) & ((g == 1) | (g == 2))) | ((chip == 3) & (g == 0))

    def goes_down(g):
        return ((chip == 0) & (g >= 1)) | ((chip == 1) & ((g == 0) | (g == 3))) | ((chip == 2) & ((g == 0) | (g == 2))) | ((chip == 3) & (g == 2))

    def own_pair(g, kind, first, on_chip):
        dst = kv.at[chip, g, kind, my_rows, :]
        recv = kv_recv.at[chip, g, core]
        return [
            remote(dst, dst, kv_send.at[g, first, kind], recv, on_chip, core),
            remote(kst.at[g, kind], dst, kv_send.at[g, first + 1, kind], recv, on_chip, other)]

    def own_copies(g, kind):
        dst = kv.at[chip, g, kind, my_rows, :]
        yield goes_up(g), own_pair(g, kind, 1, up)
        yield goes_down(g), own_pair(jnp.where((chip == 2) & (g == 2), 1, g), kind, 3, down)
        yield goes_partner(g), [remote(kst.at[g, kind], dst, kv_send.at[g, 0, kind], kv_recv.at[chip, g, core], chip, other)]

    def late_pair():
        return [copy for kind in range(2) for copy in own_pair(jnp.where(chip == 2, 3, 1), kind, 1, up)]

    def each(copies, act):
        for go, group in copies:
            @pl.when(go)
            def _():
                for copy in group:
                    act(copy)

    def kv_project(i, kind):
        g = group_at(i)
        b_ref = bv_ref if kind else bk_ref
        cols = pl.ds(pl.multiple_of(g * 256, 256), 256)
        weight = wbuf[i, :, kind * 256 : (kind + 1) * 256]
        u = (matmul_halves(hbuf, weight) + b_ref[cols].astype(F32)[None]).astype(BF16)
        even, odd = lane_blocks(u)
        if kind == 0:
            even, odd = rope(even), rope(odd)
        kv[chip, g, kind, my_rows, :] = jnp.where(core == 0, even, odd)
        kst[g, kind] = jnp.where(core == 0, odd, even)

    for kind in range(2):
        kv_load(jnp.int32(0), kind).wait()
        with jax.named_scope("kv_first"):
            kv_project(jnp.int32(0), kind)
        each(own_copies(group_at(jnp.int32(0)), kind), lambda copy: copy.start())
    wide_load(wq_hbm, 0, wqsem).start()

    @pl.loop(1, GROUPS)
    def _(i):
        for kind in range(2):
            kv_load(i, kind).wait()
        with jax.named_scope("kv_proj"):
            for kind in range(2):
                kv_project(i, kind)
        wide_load(wq_hbm, i, wqsem).start()
        for kind in range(2):
            each(own_copies(group_at(i), kind), lambda copy: copy.start())

    def wait_straight(s, g):
        for j in range(2):
            part = kv.at[s, g, :, pl.ds(j * tokens, tokens), :]
            pltpu.make_async_copy(part, part, kv_recv.at[s, g, j]).wait()

    def wait_passed(s, g):
        pltpu.make_async_copy(kv.at[s, g], kv.at[s, g], kv_recv.at[s, g, 0]).wait()

    def pass_on(s, g, to_chip, slot):
        return remote(kv.at[s, g], kv.at[s, g], fwd_send.at[slot], kv_recv.at[s, g, 0], to_chip, core)

    def q_copies(g):
        mine = qbuf.at[g, :, my_rows, :]
        away = (chip == 3) & (g == 0)
        yield jnp.logical_not(away), [
            remote(qst.at[g], mine, q_send.at[g, 0], q_recv.at[g, core], chip, other)]
        there = qbuf.at[GROUPS, :, my_rows, :]
        yield away, [
            remote(mine, there, q_send.at[g, 1], q_recv.at[GROUPS, core], up, core),
            remote(qst.at[g], there, q_send.at[g, 0], q_recv.at[GROUPS, core], up, other)]

    @pl.loop(0, GROUPS)
    def _(g):
        @pl.when(g == GROUPS - 1)
        def _():
            @pl.when(chip == 1)
            def _():
                wait_straight(2, 0)
                pass_on(2, 0, 0, 1).start()

            @pl.when(chip == 2)
            def _():
                wait_straight(1, 1)
                pass_on(1, 1, 3, 0).start()
                for copy in late_pair():
                    copy.start()

            @pl.when(chip == 3)
            def _():
                wait_straight(0, 1)
                pass_on(0, 1, 2, 0).start()

        with jax.named_scope("q_wait"):
            wide_load(wq_hbm, g, wqsem).wait()
        with jax.named_scope("q_proj"):
            heads = []
            for n in range(3):
                cols = pl.ds(pl.multiple_of(g * 768 + n * 256, 256), 256)
                u = ((matmul_halves if n == 2 else matmul_whole)(hbuf, wbuf[g, :, n * 256 : (n + 1) * 256]) + bq_ref[cols].astype(F32)[None]).astype(BF16)
                heads += [rope(part) for part in lane_blocks(u)]
            for r in range(REPS):
                even, odd = heads[r], heads[REPS + r]
                qbuf[g, r, my_rows, :] = jnp.where(core == 0, even, odd)
                qst[g, r] = jnp.where(core == 0, odd, even)
        wide_load(wo_hbm, g, wosem).start()
        each(q_copies(g), lambda copy: copy.start())

    def masked_item(q_slot, slot, s, g):
        tiles = [(r, slice(start, start + TILE)) for r in range(REPS) for start in range(0, block, TILE)]

        def score(t):
            r, at = tiles[t]
            sc = matmul_t(kv[s, g, 0, 0 : at.stop, :], qbuf[q_slot, r, at, :])
            seen = lax.broadcasted_iota(jnp.int32, (TILE, TILE), 0) <= lax.broadcasted_iota(jnp.int32, (TILE, TILE), 1)
            last = jnp.where(seen, sc[at.start :], -jnp.inf)
            return last if at.start == 0 else jnp.concatenate([sc[: at.start], last], axis=0)

        def soft(t, sc):
            r, at = tiles[t]
            parts = row_blocks(sc)
            top = jnp.max(functools.reduce(jnp.maximum, parts), axis=0, keepdims=True) * SCORE_SCALE
            top = jnp.broadcast_to(top, (8, TILE))
            probs = [jnp.exp2(part * SCORE_SCALE - top) for part in parts]
            run_max[slot, r, :, at] = top
            run_sum[slot, r, :, at] = functools.reduce(jnp.add, probs)
            return (jnp.concatenate(probs, axis=0).astype(BF16),)

        def mix(t, probs):
            r, at = tiles[t]
            mixed[slot, r, :, at] = matmul_tn(kv[s, g, 1, 0 : at.stop, :], probs)

        pipelined(len(tiles), score, soft, mix)

    def full_item(q_slot, slot, s, g):
        def score(r):
            return matmul_t(kv[s, g, 0], qbuf[q_slot, r])

        def soft(r, sc):
            parts = row_blocks(sc)
            before = run_max[slot, r]
            top = jnp.max(functools.reduce(jnp.maximum, parts), axis=0, keepdims=True) * SCORE_SCALE
            top = jnp.maximum(before, top)
            rescale = jnp.exp2(before - top)
            probs = [jnp.exp2(part * SCORE_SCALE - top) for part in parts]
            run_max[slot, r] = top
            run_sum[slot, r] = run_sum[slot, r] * rescale + functools.reduce(jnp.add, probs)
            return jnp.concatenate(probs, axis=0).astype(BF16), rescale

        def mix(r, probs, rescale):
            mixed[slot, r] = mixed[slot, r] * rescale[0:1] + matmul_tn(kv[s, g, 1], probs)

        pipelined(REPS, score, soft, mix)

    def head_cols(g, parity):
        return pl.ds(pl.multiple_of((2 * g + parity) * REPS * 128, 128), REPS * 128)

    def normalized(slot, r, rows):
        total = jnp.sum(run_sum[slot, r, :, rows], axis=0, keepdims=True)
        return jnp.transpose(mixed[slot, r, :, rows] / total).astype(BF16)

    def o_copy(g):
        return remote(ost.at[g], obuf.at[:, head_cols(g, core)], o_send.at[g], o_recv.at[g, core], chip, other)

    def finish(g):
        for r in range(REPS):
            ost[g, :, r * 128 : (r + 1) * 128] = normalized(g, r, other_rows)
        o_copy(g).start()
        for r in range(REPS):
            cols = pl.ds(pl.multiple_of(((2 * g + core) * REPS + r) * 128, 128), 128)
            obuf[:, cols] = normalized(g, r, my_rows)

    def back_copies():
        for j in range(2):
            yield remote(ost.at[GROUPS + j], obuf.at[:, head_cols(0, core)], o_send.at[GROUPS + j], o_recv.at[0, core], down, j)

    low = jnp.where(chip == 3, 1, 0)

    @pl.loop(low, jnp.where(chip == 0, GROUPS + 1, GROUPS))
    def _(i):
        g = lax.rem(i, GROUPS)

        @pl.when(i < GROUPS)
        def _():
            part = qbuf.at[i, :, other_rows, :]
            pltpu.make_async_copy(part, part, q_recv.at[i, other]).wait()
            part = kv.at[chip, g, :, other_rows, :]
            pltpu.make_async_copy(part, part, kv_recv.at[chip, g, other]).wait()

        @pl.when(i == GROUPS)
        def _():
            wait_straight(1, 3)
            pass_on(1, 3, 3, 0).start()
            wait_straight(3, 0)
            for j in range(2):
                part = qbuf.at[GROUPS, :, pl.ds(j * tokens, tokens), :]
                pltpu.make_async_copy(part, part, q_recv.at[GROUPS, j]).wait()

        with jax.named_scope('masked'):
            masked_item(i, g, jnp.where(i == GROUPS, 3, chip), g)

        @pl.when((chip == 0) & (i < GROUPS))
        def _():
            finish(i)

    def wait_o(g, parity):
        part = obuf.at[:, head_cols(g, parity)]
        pltpu.make_async_copy(part, part, o_recv.at[g, parity]).wait()

    def out_parts(n):
        for part in range(3):
            yield part, pl.ds(pl.multiple_of(n * 768 + part * 256, 256), 256)

    def out_product(n, part, g):
        at = pl.ds(pl.multiple_of(g * 768, 256), 768)
        return (matmul_halves if part == 2 else matmul_whole)(obuf.at[:, at], wbuf[n, at, part * 256 : (part + 1) * 256])

    tables = (
        ((0, 1, 2, 4, 5), (0, 0, 0, 1, 3)),
        ((0, 0, 0, 0, 4, 5), (1, 0, 2, 3, 1, 3)),
        ((1, 1, 0, 1, 0, 4, 1, 0, 5, 0), (1, 0, 1, 2, 2, 1, 3, 3, 2, 0)),
        ((0, 2, 0, 2, 1, 0, 4, 2, 1, 5, 1), (2, 1, 1, 2, 1, 3, 1, 3, 3, 3, 2)),
    )

    @pl.when(chip == 3)
    def _():
        for copy in late_pair():
            copy.start()

    @pl.loop(0, pick(chip, [len(sources) for sources, _ in tables]))
    def _(i):
        s = pick(chip, [pick(i, sources) for sources, _ in tables])
        g = pick(chip, [pick(i, groups) for _, groups in tables])
        @pl.when(s < CHIPS)
        def _():
            q_slot = jnp.where(chip == 0, GROUPS, g)
            is_passed = ((chip == 0) & (s == 2)) | ((chip == 2) & (s == 0)) | ((chip == 3) & (s == 1))
            is_here = ((chip == 0) & (s == 0)) | ((chip == 2) & (s == 1) & (g == 1)) | ((chip == 3) & (s == 0) & ((g == 1) | (g == 3)))

            with jax.named_scope("item_wait"):
                @pl.when(is_passed)
                def _():
                    wait_passed(s, g)

                @pl.when(jnp.logical_not(is_passed | is_here))
                def _():
                    wait_straight(s, g)

            @pl.when((chip == 1) & (g == 0))
            def _():
                pass_on(0, 0, 2, 0).start()

            @pl.when((chip == 2) & (s == 1) & (g == 2))
            def _():
                pass_on(1, 2, 3, 1).start()

            @pl.when((chip == 3) & (s == 0) & (g == 2))
            def _():
                pass_on(0, 2, 2, 1).start()

            @pl.when((chip == 3) & (s == 1) & (g == 1))
            def _():
                wait_straight(0, 3)
                pass_on(0, 3, 2, 2).start()

            with jax.named_scope('full'):
                full_item(q_slot, g, s, g)

            @pl.when((chip == 1) | ((chip == 2) & (s == 0)) | ((chip == 3) & (s == 1)))
            def _():
                finish(g)

            @pl.when((chip == 0) & (s == 2))
            def _():
                for j in range(2):
                    rows = pl.ds(j * tokens, tokens)
                    for r in range(REPS):
                        ost[GROUPS + j, :, r * 128 : (r + 1) * 128] = normalized(0, r, rows)
                for copy in back_copies():
                    copy.start()
                wait_straight(3, 1)
                pass_on(3, 1, 1, 1).start()

        @pl.when(s == CHIPS)
        def _():
            wait_o(1, other)

            @pl.loop(0, 4)
            def _(n):
                wide_load(wo_hbm, n, wosem).wait()
                with jax.named_scope("o_proj_a"):
                    for part, cols in out_parts(n):
                        summed[:, cols] = xbuf[:, cols].astype(F32) + out_product(n, part, 1)

        @pl.when(s == CHIPS + 1)
        def _():
            wait_o(g, other)

            @pl.loop(0, 4)
            def _(n):
                with jax.named_scope("o_proj_b"):
                    for part, cols in out_parts(n):
                        summed[:, cols] += out_product(n, part, g)

    @pl.when(chip == 1)
    def _():
        wait_straight(2, 1)
        wait_passed(3, 1)

    @pl.when(chip == 2)
    def _():
        wait_straight(3, 2)

    @pl.loop(0, GROUPS)
    def _(g):
        for kind in range(2):
            each(own_copies(g, kind), lambda copy: copy.wait_send())
        each(q_copies(g), lambda copy: copy.wait_send())

    @pl.loop(low, GROUPS)
    def _(g):
        o_copy(g).wait_send()

    @pl.when(chip == 0)
    def _():
        for copy in back_copies():
            copy.wait_send()

    @pl.when(chip >= 2)
    def _():
        for copy in late_pair():
            copy.wait_send()

    for slot in range(2):
        pass_on(0, 0, up, slot).wait_send()

    @pl.when(chip == 3)
    def _():
        pass_on(0, 0, up, 2).wait_send()

    with jax.named_scope("cache"):
        for s in range(CHIPS):
            for kind, c_ref in ((0, kc_ref), (1, vc_ref)):
                c_ref[s * block : (s + 1) * block, :] = kv[s, chip, kind]

    last_group = jnp.where(chip == 2, 3, 2)
    with jax.named_scope("o_wait"):
        wait_o(last_group, other)

        @pl.when(chip < 3)
        def _():
            wait_o(0, other)

        @pl.when(chip == 3)
        def _():
            for parity in range(2):
                wait_o(0, parity)

    @pl.loop(0, 4)
    def _(n):
        with jax.named_scope("o_proj"):
            for part, cols in out_parts(n):
                y_ref[:, cols] = (summed[:, cols] + (out_product(n, part, 0) + out_product(n, part, last_group))).astype(BF16)


def hand_over(*refs):
    sem = refs[-1]
    count = len(refs) // 2
    copies = []
    for n in range(count):
        rows = refs[n].shape[0] // 2
        for part in range(2):
            at = pl.ds(part * rows, rows)
            copies.append(pltpu.make_async_copy(refs[n].at[at], refs[count + n].at[at], sem.at[n, part]))
    for copy in copies:
        copy.start()
    for copy in copies:
        copy.wait()


def solution(mesh):
    group_size = mesh.shape['sp']
    row_spec = P(('dp', 'sp'), None)
    pos_spec = P(('dp', 'sp'))
    cache_spec = P('dp', 'sp', None)
    whole = P()

    def local(hidden, positions, norm_gain, w_q, b_q, w_k, b_k, w_v, b_v, w_o):
        tokens, width = hidden.shape
        block = 2 * tokens
        seq_len = tokens * group_size
        cosine, sine = rope_tables(positions)
        small = (norm_gain, b_q, b_k, b_v)
        anywhere = pl.BlockSpec(memory_space=pl.ANY)
        vmem = pl.BlockSpec(memory_space=pltpu.VMEM)
        dma = pltpu.SemaphoreType.DMA
        y, keys, values = pl.pallas_call(
            kernel,
            out_shape=[
                pltpu.VMEM((tokens, width), BF16),
                pltpu.VMEM((seq_len, HEAD_DIM), BF16),
                pltpu.VMEM((seq_len, HEAD_DIM), BF16),
            ],
            in_specs=[anywhere] * 11,
            out_specs=[vmem] * 3,
            scratch_shapes=[
                pltpu.VMEM((tokens, width), BF16),
                pltpu.VMEM((tokens, width), BF16),
                pltpu.VMEM((HEAD_DIM // 2, tokens), F32),
                pltpu.VMEM((HEAD_DIM // 2, tokens), F32),
                *(pltpu.VMEM(a.shape, BF16) for a in small),
                pltpu.VMEM((tokens, HEAD_DIM), F32),
                pltpu.VMEM((tokens, HEAD_DIM), F32),
                pltpu.VMEM((GROUPS, width, 768), BF16),
                pltpu.VMEM((CHIPS, GROUPS, 2, block, HEAD_DIM), BF16),
                pltpu.VMEM((GROUPS, 2, tokens, HEAD_DIM), BF16),
                pltpu.VMEM((GROUPS + 1, REPS, block, HEAD_DIM), BF16),
                pltpu.VMEM((GROUPS, REPS, tokens, HEAD_DIM), BF16),
                pltpu.VMEM((GROUPS, REPS, 8, block), F32),
                pltpu.VMEM((GROUPS, REPS, 8, block), F32),
                pltpu.VMEM((GROUPS, REPS, HEAD_DIM, block), F32),
                pltpu.VMEM((tokens, width), BF16),
                pltpu.VMEM((GROUPS + 2, tokens, REPS * HEAD_DIM), BF16),
                pltpu.VMEM((tokens, width), F32),
                dma((4,)), dma((6,)), dma((GROUPS, 2)), dma((4,)), dma((4,)),
                dma((CHIPS, GROUPS, 2)), dma((GROUPS, 5, 2)), dma((GROUPS + 1, 2)), dma((GROUPS, 2)),
                dma((GROUPS, 2)), dma((GROUPS + 2,)), dma((3,)),
            ],
            compiler_params=pltpu.CompilerParams(
                collective_id=0, has_side_effects=True, vmem_limit_bytes=62500000),
            name="block",
        )(
            hidden, cosine, sine, *small, w_q, w_k, w_v, w_o,
        )
        results = [pltpu.with_memory_space_constraint(a, pltpu.VMEM) for a in (y, keys, values)]
        y, keys, values = pl.pallas_call(
            hand_over,
            out_shape=[jax.ShapeDtypeStruct(a.shape, a.dtype) for a in results],
            in_specs=[vmem] * 3,
            out_specs=[anywhere] * 3,
            scratch_shapes=[dma((3, 2))],
            compiler_params=pltpu.CompilerParams(vmem_limit_bytes=1 << 20),
            name="hand_over",
        )(*results)
        return y, keys[:, None, :], values[:, None, :]

    return jax.shard_map(local, mesh=mesh, in_specs=(row_spec, pos_spec, whole, whole, whole, whole, whole, whole, whole, whole), out_specs=(row_spec, cache_spec, cache_spec), check_vma=False)
```

```python
import functools
import math

import jax
import jax.numpy as jnp
import numpy as np
from jax import lax
from jax.experimental import pallas as pl
from jax.experimental.pallas import tpu as pltpu
from jax.sharding import PartitionSpec as P

HEAD_DIM = 128
ROPE_BASE = 1000000.0
NORM_EPS = 1e-6
SCORE_SCALE = math.log2(math.e) / math.sqrt(HEAD_DIM)
CHIPS = 4
GROUPS = 4
REPS = 3
TILE = 384
BF16 = jnp.bfloat16
F32 = jnp.float32


def matmul(a, b):
    return lax.dot_general(a, b, (((1,), (0,)), ((), ())), preferred_element_type=F32)


def matmul_t(a, b):
    return lax.dot_general(a, b, (((1,), (1,)), ((), ())), preferred_element_type=F32)


def matmul_tn(a, b):
    return lax.dot_general(a, b, (((0,), (0,)), ((), ())), preferred_element_type=F32)


def matmul_halves(a_ref, b):
    half = a_ref.shape[0] // 2
    return jnp.concatenate([matmul(a_ref[:half], b), matmul(a_ref[half:], b)], axis=0)


def matmul_whole(a_ref, b):
    return matmul(a_ref[...], b)


def pick(i, values):
    out = values[-1]
    for n in range(len(values) - 1):
        out = jnp.where(i == n, values[n], out)
    return out


def lane_blocks(x):
    return [x[:, i : i + 128] for i in range(0, x.shape[1], 128)]


def row_blocks(x):
    return [x[i : i + 8] for i in range(0, x.shape[0], 8)]


def pipelined(count, score, soft, mix):
    scores, weights = {}, {}
    for t in range(count + 2):
        if t < count:
            scores[t] = score(t)
        if 0 <= t - 1 < count:
            weights[t - 1] = soft(t - 1, scores.pop(t - 1))
        if 0 <= t - 2 < count:
            mix(t - 2, *weights.pop(t - 2))


def kernel(
    x_hbm, pos_hbm, freq_hbm, gain_hbm, bq_hbm, bk_hbm, bv_hbm, wq_hbm, wk_hbm, wv_hbm, wo_hbm,
    y_ref, kc_ref, vc_ref,
    xbuf, hbuf, pos_ref, freq_ref, gain_ref, bq_ref, bk_ref, bv_ref, cos_ref, sin_ref, wbuf, kv, kst, qbuf, qst, run_max, run_sum, mixed, obuf, ost, summed,
    xsem, smallsem, wkvsem, wqsem, wosem,
    kv_recv, kv_send, q_recv, q_send, o_recv, o_send, fwd_send,
):
    me = lax.axis_index("sp")
    chip = lax.div(me, 2)
    core = lax.rem(me, 2)
    other = 1 - core
    up = lax.rem(chip + 1, CHIPS)
    down = lax.rem(chip + CHIPS - 1, CHIPS)
    tokens = xbuf.shape[0]
    block = 2 * tokens
    my_rows = pl.ds(pl.multiple_of(core * tokens, 128), tokens)
    other_rows = pl.ds(pl.multiple_of(other * tokens, 128), tokens)

    def is_chip(n):
        return chip == n

    def device(on_chip, on_core):
        return {"sp": on_chip * 2 + on_core}

    def remote(src, dst, send_sem, recv_sem, on_chip, on_core):
        return pltpu.make_async_remote_copy(
            src_ref=src, dst_ref=dst, send_sem=send_sem, recv_sem=recv_sem,
            device_id=device(on_chip, on_core), device_id_type=pl.DeviceIdType.MESH,
        )

    barrier = pltpu.get_barrier_semaphore()
    for on_chip, on_core in ((chip, other), (up, core), (up, other), (down, core), (down, other)):
        pl.semaphore_signal(barrier, inc=1, device_id=device(on_chip, on_core), device_id_type=pl.DeviceIdType.MESH)

    def group_at(i):
        return jnp.where((chip < 3) & (i < 2), 1 - i, i)

    def kv_load(i, kind):
        w_hbm = wk_hbm if kind == 0 else wv_hbm
        cols = pl.ds(pl.multiple_of(group_at(i) * 256, 256), 256)
        return pltpu.make_async_copy(
            w_hbm.at[:, cols], wbuf.at[i, :, kind * 256 : (kind + 1) * 256], wkvsem.at[i, kind])

    def wide_load(w_hbm, g, sem):
        cols = pl.ds(pl.multiple_of(g * 768, 256), 768)
        return pltpu.make_async_copy(w_hbm.at[:, cols], wbuf.at[g], sem.at[g])

    def x_copy(n):
        rows = pl.ds(n * (tokens // 4), tokens // 4)
        return pltpu.make_async_copy(x_hbm.at[rows], xbuf.at[rows], xsem.at[n])

    small_copies = [
        pltpu.make_async_copy(src, dst, smallsem.at[n])
        for n, (src, dst) in enumerate((
            (gain_hbm, gain_ref), (bk_hbm, bk_ref), (bv_hbm, bv_ref), (bq_hbm, bq_ref), (pos_hbm, pos_ref), (freq_hbm, freq_ref)))
    ]
    x_copy(0).start()
    small_copies[0].start()
    x_copy(1).start()
    for kind in (1, 0):
        kv_load(jnp.int32(0), kind).start()
    for n in range(2, 4):
        x_copy(n).start()
    for copy in small_copies[1:]:
        copy.start()
    small_copies[0].wait()
    gain = gain_ref[...].astype(F32)[None]
    for n in range(4):
        with jax.named_scope("x_wait"):
            x_copy(n).wait()
        if n == 1:
            for i in range(1, GROUPS):
                for kind in range(2):
                    kv_load(jnp.int32(i), kind).start()
        for start in range(n * (tokens // 4), (n + 1) * (tokens // 4), 16):
            wide = xbuf[start : start + 16, :].astype(F32)
            inv_rms = lax.rsqrt(jnp.mean(wide * wide, axis=-1, keepdims=True) + NORM_EPS)
            hbuf[start : start + 16, :] = (wide * inv_rms * gain).astype(BF16)

    for copy in small_copies[1:]:
        copy.wait()
    with jax.named_scope("entry"):
        pl.semaphore_wait(barrier, 5)

    def rope_tables():
        freq = jnp.transpose(jnp.broadcast_to(freq_ref[...][None], (128, HEAD_DIM // 2)))
        positions = pos_ref[...].astype(F32)[None]
        for start in range(0, tokens, 128):
            angle = positions[:, start : start + 128] * freq
            cosine, sine = jnp.cos(angle), jnp.sin(angle)
            cos_ref[start : start + 128, :] = jnp.transpose(jnp.concatenate([cosine, cosine], axis=0))
            sin_ref[start : start + 128, :] = jnp.transpose(jnp.concatenate([-sine, sine], axis=0))

    def rope(u):
        wide = u.astype(F32)
        return (wide * cos_ref[...] + pltpu.roll(wide, HEAD_DIM // 2, 1) * sin_ref[...]).astype(BF16)

    def goes_partner(g):
        return jnp.logical_not((chip == 3) & (g == 0))

    def goes_up(g):
        return (chip <= 1) | ((chip == 2) & ((g == 1) | (g == 2))) | ((chip == 3) & (g == 0))

    def goes_down(g):
        return ((chip == 0) & (g >= 1)) | ((chip == 1) & ((g == 0) | (g == 3))) | ((chip == 2) & ((g == 0) | (g == 2))) | ((chip == 3) & (g == 2))

    def own_pair(g, kind, first, on_chip):
        dst = kv.at[chip, g, kind, my_rows, :]
        recv = kv_recv.at[chip, g, core]
        return [
            remote(dst, dst, kv_send.at[g, first, kind], recv, on_chip, core),
            remote(kst.at[g, kind], dst, kv_send.at[g, first + 1, kind], recv, on_chip, other)]

    def own_copies(g, kind):
        dst = kv.at[chip, g, kind, my_rows, :]
        yield goes_up(g), own_pair(g, kind, 1, up)
        yield goes_down(g), own_pair(jnp.where((chip == 2) & (g == 2), 1, g), kind, 3, down)
        yield goes_partner(g), [remote(kst.at[g, kind], dst, kv_send.at[g, 0, kind], kv_recv.at[chip, g, core], chip, other)]

    def late_pair():
        return [copy for kind in range(2) for copy in own_pair(jnp.where(chip == 2, 3, 1), kind, 1, up)]

    def each(copies, act):
        for go, group in copies:
            @pl.when(go)
            def _():
                for copy in group:
                    act(copy)

    def kv_project(i, kind):
        g = group_at(i)
        b_ref = bv_ref if kind else bk_ref
        cols = pl.ds(pl.multiple_of(g * 256, 256), 256)
        weight = wbuf[i, :, kind * 256 : (kind + 1) * 256]
        u = (matmul_halves(hbuf, weight) + b_ref[cols].astype(F32)[None]).astype(BF16)
        even, odd = lane_blocks(u)
        if kind == 0:
            even, odd = rope(even), rope(odd)
        kv[chip, g, kind, my_rows, :] = jnp.where(core == 0, even, odd)
        kst[g, kind] = jnp.where(core == 0, odd, even)

    for kind in (1, 0):
        kv_load(jnp.int32(0), kind).wait()
        with jax.named_scope("kv_first"):
            if kind == 1:
                rope_tables()
            kv_project(jnp.int32(0), kind)
        each(own_copies(group_at(jnp.int32(0)), kind), lambda copy: copy.start())
    wide_load(wq_hbm, 0, wqsem).start()

    @pl.loop(1, GROUPS)
    def _(i):
        for kind in range(2):
            kv_load(i, kind).wait()
        with jax.named_scope("kv_proj"):
            for kind in range(2):
                kv_project(i, kind)
        wide_load(wq_hbm, i, wqsem).start()
        for kind in range(2):
            each(own_copies(group_at(i), kind), lambda copy: copy.start())

    def wait_straight(s, g):
        for j in range(2):
            part = kv.at[s, g, :, pl.ds(j * tokens, tokens), :]
            pltpu.make_async_copy(part, part, kv_recv.at[s, g, j]).wait()

    def wait_passed(s, g):
        pltpu.make_async_copy(kv.at[s, g], kv.at[s, g], kv_recv.at[s, g, 0]).wait()

    def pass_on(s, g, to_chip, slot):
        return remote(kv.at[s, g], kv.at[s, g], fwd_send.at[slot], kv_recv.at[s, g, 0], to_chip, core)

    def q_copies(g):
        mine = qbuf.at[g, :, my_rows, :]
        away = (chip == 3) & (g == 0)
        yield jnp.logical_not(away), [
            remote(qst.at[g], mine, q_send.at[g, 0], q_recv.at[g, core], chip, other)]
        there = qbuf.at[GROUPS, :, my_rows, :]
        yield away, [
            remote(mine, there, q_send.at[g, 1], q_recv.at[GROUPS, core], up, core),
            remote(qst.at[g], there, q_send.at[g, 0], q_recv.at[GROUPS, core], up, other)]

    @pl.loop(0, GROUPS)
    def _(g):
        @pl.when(g == GROUPS - 1)
        def _():
            @pl.when(chip == 1)
            def _():
                wait_straight(2, 0)
                pass_on(2, 0, 0, 1).start()

            @pl.when(chip == 2)
            def _():
                wait_straight(1, 1)
                pass_on(1, 1, 3, 0).start()
                for copy in late_pair():
                    copy.start()

            @pl.when(chip == 3)
            def _():
                wait_straight(0, 1)
                pass_on(0, 1, 2, 0).start()

        with jax.named_scope("q_wait"):
            wide_load(wq_hbm, g, wqsem).wait()
        with jax.named_scope("q_proj"):
            heads = []
            for n in range(3):
                cols = pl.ds(pl.multiple_of(g * 768 + n * 256, 256), 256)
                u = ((matmul_halves if n == 2 else matmul_whole)(hbuf, wbuf[g, :, n * 256 : (n + 1) * 256]) + bq_ref[cols].astype(F32)[None]).astype(BF16)
                heads += [rope(part) for part in lane_blocks(u)]
            for r in range(REPS):
                even, odd = heads[r], heads[REPS + r]
                qbuf[g, r, my_rows, :] = jnp.where(core == 0, even, odd)
                qst[g, r] = jnp.where(core == 0, odd, even)
        wide_load(wo_hbm, g, wosem).start()
        each(q_copies(g), lambda copy: copy.start())

    def masked_item(q_slot, slot, s, g):
        tiles = [(r, slice(start, start + TILE)) for r in range(REPS) for start in range(0, block, TILE)]

        def score(t):
            r, at = tiles[t]
            sc = matmul_t(kv[s, g, 0, 0 : at.stop, :], qbuf[q_slot, r, at, :])
            seen = lax.broadcasted_iota(jnp.int32, (TILE, TILE), 0) <= lax.broadcasted_iota(jnp.int32, (TILE, TILE), 1)
            last = jnp.where(seen, sc[at.start :], -jnp.inf)
            return last if at.start == 0 else jnp.concatenate([sc[: at.start], last], axis=0)

        def soft(t, sc):
            r, at = tiles[t]
            parts = row_blocks(sc)
            top = jnp.max(functools.reduce(jnp.maximum, parts), axis=0, keepdims=True) * SCORE_SCALE
            top = jnp.broadcast_to(top, (8, TILE))
            probs = [jnp.exp2(part * SCORE_SCALE - top) for part in parts]
            run_max[slot, r, :, at] = top
            run_sum[slot, r, :, at] = functools.reduce(jnp.add, probs)
            return (jnp.concatenate(probs, axis=0).astype(BF16),)

        def mix(t, probs):
            r, at = tiles[t]
            mixed[slot, r, :, at] = matmul_tn(kv[s, g, 1, 0 : at.stop, :], probs)

        pipelined(len(tiles), score, soft, mix)

    def full_item(q_slot, slot, s, g):
        def score(r):
            return matmul_t(kv[s, g, 0], qbuf[q_slot, r])

        def soft(r, sc):
            parts = row_blocks(sc)
            before = run_max[slot, r]
            top = jnp.max(functools.reduce(jnp.maximum, parts), axis=0, keepdims=True) * SCORE_SCALE
            top = jnp.maximum(before, top)
            rescale = jnp.exp2(before - top)
            probs = [jnp.exp2(part * SCORE_SCALE - top) for part in parts]
            run_max[slot, r] = top
            run_sum[slot, r] = run_sum[slot, r] * rescale + functools.reduce(jnp.add, probs)
            return jnp.concatenate(probs, axis=0).astype(BF16), rescale

        def mix(r, probs, rescale):
            mixed[slot, r] = mixed[slot, r] * rescale[0:1] + matmul_tn(kv[s, g, 1], probs)

        pipelined(REPS, score, soft, mix)

    def head_cols(g, parity):
        return pl.ds(pl.multiple_of((2 * g + parity) * REPS * 128, 128), REPS * 128)

    def normalized(slot, r, rows):
        total = jnp.sum(run_sum[slot, r, :, rows], axis=0, keepdims=True)
        return jnp.transpose(mixed[slot, r, :, rows] / total).astype(BF16)

    def o_copy(g):
        return remote(ost.at[g], obuf.at[:, head_cols(g, core)], o_send.at[g], o_recv.at[g, core], chip, other)

    def finish(g):
        for r in range(REPS):
            ost[g, :, r * 128 : (r + 1) * 128] = normalized(g, r, other_rows)
        o_copy(g).start()
        for r in range(REPS):
            cols = pl.ds(pl.multiple_of(((2 * g + core) * REPS + r) * 128, 128), 128)
            obuf[:, cols] = normalized(g, r, my_rows)

    def back_copies():
        for j in range(2):
            yield remote(ost.at[GROUPS + j], obuf.at[:, head_cols(0, core)], o_send.at[GROUPS + j], o_recv.at[0, core], down, j)

    low = jnp.where(chip == 3, 1, 0)

    @pl.loop(low, jnp.where(chip == 0, GROUPS + 1, GROUPS))
    def _(i):
        g = lax.rem(i, GROUPS)

        @pl.when(i < GROUPS)
        def _():
            part = qbuf.at[i, :, other_rows, :]
            pltpu.make_async_copy(part, part, q_recv.at[i, other]).wait()
            part = kv.at[chip, g, :, other_rows, :]
            pltpu.make_async_copy(part, part, kv_recv.at[chip, g, other]).wait()

        @pl.when(i == GROUPS)
        def _():
            wait_straight(1, 3)
            pass_on(1, 3, 3, 0).start()
            wait_straight(3, 0)
            for j in range(2):
                part = qbuf.at[GROUPS, :, pl.ds(j * tokens, tokens), :]
                pltpu.make_async_copy(part, part, q_recv.at[GROUPS, j]).wait()

        with jax.named_scope('masked'):
            masked_item(i, g, jnp.where(i == GROUPS, 3, chip), g)

        @pl.when((chip == 0) & (i < GROUPS))
        def _():
            finish(i)

    def wait_o(g, parity):
        part = obuf.at[:, head_cols(g, parity)]
        pltpu.make_async_copy(part, part, o_recv.at[g, parity]).wait()

    def out_parts(n):
        for part in range(3):
            yield part, pl.ds(pl.multiple_of(n * 768 + part * 256, 256), 256)

    def out_product(n, part, g):
        at = pl.ds(pl.multiple_of(g * 768, 256), 768)
        return (matmul_halves if part == 2 else matmul_whole)(obuf.at[:, at], wbuf[n, at, part * 256 : (part + 1) * 256])

    tables = (
        ((0, 1, 2, 4, 5), (0, 0, 0, 1, 3)),
        ((0, 0, 0, 0, 4, 5), (1, 0, 2, 3, 1, 3)),
        ((1, 1, 0, 1, 0, 4, 1, 0, 5, 0), (1, 0, 1, 2, 2, 1, 3, 3, 2, 0)),
        ((0, 2, 0, 2, 1, 0, 4, 2, 1, 5, 1), (2, 1, 1, 2, 1, 3, 1, 3, 3, 3, 2)),
    )

    @pl.when(chip == 3)
    def _():
        for copy in late_pair():
            copy.start()

    @pl.loop(0, pick(chip, [len(sources) for sources, _ in tables]))
    def _(i):
        s = pick(chip, [pick(i, sources) for sources, _ in tables])
        g = pick(chip, [pick(i, groups) for _, groups in tables])
        @pl.when(s < CHIPS)
        def _():
            q_slot = jnp.where(chip == 0, GROUPS, g)
            is_passed = ((chip == 0) & (s == 2)) | ((chip == 2) & (s == 0)) | ((chip == 3) & (s == 1))
            is_here = ((chip == 0) & (s == 0)) | ((chip == 2) & (s == 1) & (g == 1)) | ((chip == 3) & (s == 0) & ((g == 1) | (g == 3)))

            with jax.named_scope("item_wait"):
                @pl.when(is_passed)
                def _():
                    wait_passed(s, g)

                @pl.when(jnp.logical_not(is_passed | is_here))
                def _():
                    wait_straight(s, g)

            @pl.when((chip == 1) & (g == 0))
            def _():
                pass_on(0, 0, 2, 0).start()

            @pl.when((chip == 2) & (s == 1) & (g == 2))
            def _():
                pass_on(1, 2, 3, 1).start()

            @pl.when((chip == 3) & (s == 0) & (g == 2))
            def _():
                pass_on(0, 2, 2, 1).start()

            @pl.when((chip == 3) & (s == 1) & (g == 1))
            def _():
                wait_straight(0, 3)
                pass_on(0, 3, 2, 2).start()

            with jax.named_scope('full'):
                full_item(q_slot, g, s, g)

            @pl.when((chip == 1) | ((chip == 2) & (s == 0)) | ((chip == 3) & (s == 1)))
            def _():
                finish(g)

            @pl.when((chip == 0) & (s == 2))
            def _():
                for j in range(2):
                    rows = pl.ds(j * tokens, tokens)
                    for r in range(REPS):
                        ost[GROUPS + j, :, r * 128 : (r + 1) * 128] = normalized(0, r, rows)
                for copy in back_copies():
                    copy.start()
                wait_straight(3, 1)
                pass_on(3, 1, 1, 1).start()

        @pl.when(s == CHIPS)
        def _():
            wait_o(1, other)

            @pl.loop(0, 4)
            def _(n):
                wide_load(wo_hbm, n, wosem).wait()
                with jax.named_scope("o_proj_a"):
                    for part, cols in out_parts(n):
                        summed[:, cols] = xbuf[:, cols].astype(F32) + out_product(n, part, 1)

        @pl.when(s == CHIPS + 1)
        def _():
            wait_o(g, other)

            @pl.loop(0, 4)
            def _(n):
                with jax.named_scope("o_proj_b"):
                    for part, cols in out_parts(n):
                        summed[:, cols] += out_product(n, part, g)

    @pl.when(chip == 1)
    def _():
        wait_straight(2, 1)
        wait_passed(3, 1)

    @pl.when(chip == 2)
    def _():
        wait_straight(3, 2)

    @pl.loop(0, GROUPS)
    def _(g):
        for kind in range(2):
            each(own_copies(g, kind), lambda copy: copy.wait_send())
        each(q_copies(g), lambda copy: copy.wait_send())

    @pl.loop(low, GROUPS)
    def _(g):
        o_copy(g).wait_send()

    @pl.when(chip == 0)
    def _():
        for copy in back_copies():
            copy.wait_send()

    @pl.when(chip >= 2)
    def _():
        for copy in late_pair():
            copy.wait_send()

    for slot in range(2):
        pass_on(0, 0, up, slot).wait_send()

    @pl.when(chip == 3)
    def _():
        pass_on(0, 0, up, 2).wait_send()

    with jax.named_scope("cache"):
        for s in range(CHIPS):
            for kind, c_ref in ((0, kc_ref), (1, vc_ref)):
                c_ref[s * block : (s + 1) * block, :] = kv[s, chip, kind]

    last_group = jnp.where(chip == 2, 3, 2)
    with jax.named_scope("o_wait"):
        wait_o(last_group, other)

        @pl.when(chip < 3)
        def _():
            wait_o(0, other)

        @pl.when(chip == 3)
        def _():
            for parity in range(2):
                wait_o(0, parity)

    @pl.loop(0, 4)
    def _(n):
        with jax.named_scope("o_proj"):
            for part, cols in out_parts(n):
                y_ref[:, cols] = (summed[:, cols] + (out_product(n, part, 0) + out_product(n, part, last_group))).astype(BF16)


def hand_over(*refs):
    sem = refs[-1]
    count = len(refs) // 2
    copies = []
    for n in range(count):
        rows = refs[n].shape[0] // 2
        for part in range(2):
            at = pl.ds(part * rows, rows)
            copies.append(pltpu.make_async_copy(refs[n].at[at], refs[count + n].at[at], sem.at[n, part]))
    for copy in copies:
        copy.start()
    for copy in copies:
        copy.wait()


def solution(mesh):
    group_size = mesh.shape['sp']
    row_spec = P(('dp', 'sp'), None)
    pos_spec = P(('dp', 'sp'))
    cache_spec = P('dp', 'sp', None)
    whole = P()

    def local(hidden, positions, norm_gain, w_q, b_q, w_k, b_k, w_v, b_v, w_o):
        tokens, width = hidden.shape
        block = 2 * tokens
        seq_len = tokens * group_size
        inv_freq = jnp.asarray(np.float32(ROPE_BASE) ** (np.float32(-2.0) * np.arange(HEAD_DIM // 2, dtype=np.float32) / np.float32(HEAD_DIM)))
        small = (norm_gain, b_q, b_k, b_v)
        anywhere = pl.BlockSpec(memory_space=pl.ANY)
        vmem = pl.BlockSpec(memory_space=pltpu.VMEM)
        dma = pltpu.SemaphoreType.DMA
        y, keys, values = pl.pallas_call(
            kernel,
            out_shape=[
                pltpu.VMEM((tokens, width), BF16),
                pltpu.VMEM((seq_len, HEAD_DIM), BF16),
                pltpu.VMEM((seq_len, HEAD_DIM), BF16),
            ],
            in_specs=[anywhere] * 11,
            out_specs=[vmem] * 3,
            scratch_shapes=[
                pltpu.VMEM((tokens, width), BF16),
                pltpu.VMEM((tokens, width), BF16),
                pltpu.VMEM((tokens,), jnp.int32),
                pltpu.VMEM((HEAD_DIM // 2,), F32),
                *(pltpu.VMEM(a.shape, BF16) for a in small),
                pltpu.VMEM((tokens, HEAD_DIM), F32),
                pltpu.VMEM((tokens, HEAD_DIM), F32),
                pltpu.VMEM((GROUPS, width, 768), BF16),
                pltpu.VMEM((CHIPS, GROUPS, 2, block, HEAD_DIM), BF16),
                pltpu.VMEM((GROUPS, 2, tokens, HEAD_DIM), BF16),
                pltpu.VMEM((GROUPS + 1, REPS, block, HEAD_DIM), BF16),
                pltpu.VMEM((GROUPS, REPS, tokens, HEAD_DIM), BF16),
                pltpu.VMEM((GROUPS, REPS, 8, block), F32),
                pltpu.VMEM((GROUPS, REPS, 8, block), F32),
                pltpu.VMEM((GROUPS, REPS, HEAD_DIM, block), F32),
                pltpu.VMEM((tokens, width), BF16),
                pltpu.VMEM((GROUPS + 2, tokens, REPS * HEAD_DIM), BF16),
                pltpu.VMEM((tokens, width), F32),
                dma((4,)), dma((6,)), dma((GROUPS, 2)), dma((4,)), dma((4,)),
                dma((CHIPS, GROUPS, 2)), dma((GROUPS, 5, 2)), dma((GROUPS + 1, 2)), dma((GROUPS, 2)),
                dma((GROUPS, 2)), dma((GROUPS + 2,)), dma((3,)),
            ],
            compiler_params=pltpu.CompilerParams(
                collective_id=0, has_side_effects=True, vmem_limit_bytes=62500000),
            name="block",
        )(
            hidden, positions, inv_freq, *small, w_q, w_k, w_v, w_o,
        )
        results = [pltpu.with_memory_space_constraint(a, pltpu.VMEM) for a in (y, keys, values)]
        y, keys, values = pl.pallas_call(
            hand_over,
            out_shape=[jax.ShapeDtypeStruct(a.shape, a.dtype) for a in results],
            in_specs=[vmem] * 3,
            out_specs=[anywhere] * 3,
            scratch_shapes=[dma((3, 2))],
            compiler_params=pltpu.CompilerParams(vmem_limit_bytes=1 << 20),
            name="hand_over",
        )(*results)
        return y, keys[:, None, :], values[:, None, :]

    return jax.shard_map(local, mesh=mesh, in_specs=(row_spec, pos_spec, whole, whole, whole, whole, whole, whole, whole, whole), out_specs=(row_spec, cache_spec, cache_spec), check_vma=False)
```

```python
import functools
import math

import jax
import jax.numpy as jnp
import numpy as np
from jax import lax
from jax.experimental import pallas as pl
from jax.experimental.pallas import tpu as pltpu
from jax.sharding import PartitionSpec as P

HEAD_DIM = 128
ROPE_BASE = 1000000.0
NORM_EPS = 1e-6
SCORE_SCALE = math.log2(math.e) / math.sqrt(HEAD_DIM)
CHIPS = 4
GROUPS = 4
REPS = 3
TILE = 384
BF16 = jnp.bfloat16
F32 = jnp.float32


def matmul(a, b):
    return lax.dot_general(a, b, (((1,), (0,)), ((), ())), preferred_element_type=F32)


def matmul_t(a, b):
    return lax.dot_general(a, b, (((1,), (1,)), ((), ())), preferred_element_type=F32)


def matmul_tn(a, b):
    return lax.dot_general(a, b, (((0,), (0,)), ((), ())), preferred_element_type=F32)


def matmul_halves(a_ref, b):
    half = a_ref.shape[0] // 2
    return jnp.concatenate([matmul(a_ref[:half], b), matmul(a_ref[half:], b)], axis=0)


def matmul_whole(a_ref, b):
    return matmul(a_ref[...], b)


def pick(i, values):
    out = values[-1]
    for n in range(len(values) - 1):
        out = jnp.where(i == n, values[n], out)
    return out


def lane_blocks(x):
    return [x[:, i : i + 128] for i in range(0, x.shape[1], 128)]


def row_blocks(x):
    return [x[i : i + 8] for i in range(0, x.shape[0], 8)]


def pipelined(count, score, soft, mix):
    scores, weights = {}, {}
    for t in range(count + 2):
        if t < count:
            scores[t] = score(t)
        if 0 <= t - 1 < count:
            weights[t - 1] = soft(t - 1, scores.pop(t - 1))
        if 0 <= t - 2 < count:
            mix(t - 2, *weights.pop(t - 2))


def kernel(
    x_hbm, pos_hbm, freq_hbm, gain_hbm, bq_hbm, bk_hbm, bv_hbm, wq_hbm, wk_hbm, wv_hbm, wo_hbm,
    y_ref, kc_ref, vc_ref,
    xbuf, hbuf, pos_ref, freq_ref, gain_ref, bq_ref, bk_ref, bv_ref, cos_ref, sin_ref, wbuf, kv, kst, qbuf, qst, run_max, run_sum, mixed, obuf, ost, summed,
    xsem, smallsem, wkvsem, wqsem, wosem,
    kv_recv, kv_send, q_recv, q_send, o_recv, o_send, fwd_send,
):
    me = lax.axis_index("sp")
    chip = lax.div(me, 2)
    core = lax.rem(me, 2)
    other = 1 - core
    up = lax.rem(chip + 1, CHIPS)
    down = lax.rem(chip + CHIPS - 1, CHIPS)
    tokens = xbuf.shape[0]
    block = 2 * tokens
    my_rows = pl.ds(pl.multiple_of(core * tokens, 128), tokens)
    other_rows = pl.ds(pl.multiple_of(other * tokens, 128), tokens)

    def is_chip(n):
        return chip == n

    def device(on_chip, on_core):
        return {"sp": on_chip * 2 + on_core}

    def remote(src, dst, send_sem, recv_sem, on_chip, on_core):
        return pltpu.make_async_remote_copy(
            src_ref=src, dst_ref=dst, send_sem=send_sem, recv_sem=recv_sem,
            device_id=device(on_chip, on_core), device_id_type=pl.DeviceIdType.MESH,
        )

    barrier = pltpu.get_barrier_semaphore()
    for on_chip, on_core in ((chip, other), (up, core), (up, other), (down, core), (down, other)):
        pl.semaphore_signal(barrier, inc=1, device_id=device(on_chip, on_core), device_id_type=pl.DeviceIdType.MESH)

    def group_at(i):
        return jnp.where((chip < 3) & (i < 2), 1 - i, i)

    def kv_load(i, kind):
        w_hbm = wk_hbm if kind == 0 else wv_hbm
        cols = pl.ds(pl.multiple_of(group_at(i) * 256, 256), 256)
        return pltpu.make_async_copy(
            w_hbm.at[:, cols], wbuf.at[i, :, kind * 256 : (kind + 1) * 256], wkvsem.at[i, kind])

    def wide_load(w_hbm, g, sem):
        cols = pl.ds(pl.multiple_of(g * 768, 256), 768)
        return pltpu.make_async_copy(w_hbm.at[:, cols], wbuf.at[g], sem.at[g])

    def x_copy(n):
        rows = pl.ds(n * (tokens // 4), tokens // 4)
        return pltpu.make_async_copy(x_hbm.at[rows], xbuf.at[rows], xsem.at[n])

    small_copies = [
        pltpu.make_async_copy(src, dst, smallsem.at[n])
        for n, (src, dst) in enumerate((
            (gain_hbm, gain_ref), (bk_hbm, bk_ref), (bv_hbm, bv_ref), (bq_hbm, bq_ref), (pos_hbm, pos_ref), (freq_hbm, freq_ref)))
    ]
    x_copy(0).start()
    small_copies[0].start()
    x_copy(1).start()
    for kind in (1, 0):
        kv_load(jnp.int32(0), kind).start()
    for n in range(2, 4):
        x_copy(n).start()
    for copy in small_copies[1:]:
        copy.start()
    small_copies[0].wait()
    gain = gain_ref[...].astype(F32)[None]
    for n in range(4):
        with jax.named_scope("x_wait"):
            x_copy(n).wait()
        if n == 1:
            for i in range(1, GROUPS):
                for kind in range(2):
                    kv_load(jnp.int32(i), kind).start()
        for start in range(n * (tokens // 4), (n + 1) * (tokens // 4), 16):
            wide = xbuf[start : start + 16, :].astype(F32)
            inv_rms = lax.rsqrt(jnp.mean(wide * wide, axis=-1, keepdims=True) + NORM_EPS)
            hbuf[start : start + 16, :] = (wide * inv_rms * gain).astype(BF16)

    for copy in small_copies[1:]:
        copy.wait()
    with jax.named_scope("entry"):
        pl.semaphore_wait(barrier, 5)

    def rope_tables():
        freq = jnp.transpose(jnp.broadcast_to(freq_ref[...][None], (128, HEAD_DIM // 2)))
        positions = pos_ref[...].astype(F32)[None]
        for start in range(0, tokens, 128):
            angle = positions[:, start : start + 128] * freq
            cosine, sine = jnp.cos(angle), jnp.sin(angle)
            cos_ref[start : start + 128, :] = jnp.transpose(jnp.concatenate([cosine, cosine], axis=0))
            sin_ref[start : start + 128, :] = jnp.transpose(jnp.concatenate([-sine, sine], axis=0))

    def rope(u):
        wide = u.astype(F32)
        return (wide * cos_ref[...] + pltpu.roll(wide, HEAD_DIM // 2, 1) * sin_ref[...]).astype(BF16)

    def goes_partner(g):
        return jnp.logical_not((chip == 3) & (g == 0))

    def goes_up(g):
        return (chip <= 1) | ((chip == 2) & ((g == 1) | (g == 2))) | ((chip == 3) & (g == 0))

    def goes_down(g):
        return ((chip == 0) & (g >= 1)) | ((chip == 1) & ((g == 0) | (g == 3))) | ((chip == 2) & ((g == 0) | (g == 2))) | ((chip == 3) & (g == 2))

    def own_pair(g, kind, first, on_chip):
        dst = kv.at[chip, g, kind, my_rows, :]
        recv = kv_recv.at[chip, g, core]
        return [
            remote(dst, dst, kv_send.at[g, first, kind], recv, on_chip, core),
            remote(kst.at[g, kind], dst, kv_send.at[g, first + 1, kind], recv, on_chip, other)]

    def own_copies(g, kind):
        dst = kv.at[chip, g, kind, my_rows, :]
        yield goes_up(g), own_pair(g, kind, 1, up)
        yield goes_down(g), own_pair(jnp.where((chip == 2) & (g == 2), 1, g), kind, 3, down)
        yield goes_partner(g), [remote(kst.at[g, kind], dst, kv_send.at[g, 0, kind], kv_recv.at[chip, g, core], chip, other)]

    def late_pair():
        return [copy for kind in range(2) for copy in own_pair(jnp.where(chip == 2, 3, 1), kind, 1, up)]

    def each(copies, act):
        for go, group in copies:
            @pl.when(go)
            def _():
                for copy in group:
                    act(copy)

    def kv_project(i, kind):
        g = group_at(i)
        b_ref = bv_ref if kind else bk_ref
        cols = pl.ds(pl.multiple_of(g * 256, 256), 256)
        weight = wbuf[i, :, kind * 256 : (kind + 1) * 256]
        u = (matmul_halves(hbuf, weight) + b_ref[cols].astype(F32)[None]).astype(BF16)
        even, odd = lane_blocks(u)
        if kind == 0:
            even, odd = rope(even), rope(odd)
        kv[chip, g, kind, my_rows, :] = jnp.where(core == 0, even, odd)
        kst[g, kind] = jnp.where(core == 0, odd, even)

    for kind in (1, 0):
        kv_load(jnp.int32(0), kind).wait()
        with jax.named_scope("kv_first"):
            if kind == 1:
                rope_tables()
            kv_project(jnp.int32(0), kind)
        each(own_copies(group_at(jnp.int32(0)), kind), lambda copy: copy.start())
    wide_load(wq_hbm, 0, wqsem).start()

    @pl.loop(1, GROUPS)
    def _(i):
        for kind in range(2):
            kv_load(i, kind).wait()
        with jax.named_scope("kv_proj"):
            for kind in range(2):
                kv_project(i, kind)
        wide_load(wq_hbm, i, wqsem).start()
        for kind in range(2):
            each(own_copies(group_at(i), kind), lambda copy: copy.start())

    def wait_straight(s, g):
        for j in range(2):
            part = kv.at[s, g, :, pl.ds(j * tokens, tokens), :]
            pltpu.make_async_copy(part, part, kv_recv.at[s, g, j]).wait()

    def wait_passed(s, g):
        pltpu.make_async_copy(kv.at[s, g], kv.at[s, g], kv_recv.at[s, g, 0]).wait()

    def pass_on(s, g, to_chip, slot):
        return remote(kv.at[s, g], kv.at[s, g], fwd_send.at[slot], kv_recv.at[s, g, 0], to_chip, core)

    def q_copies(g):
        mine = qbuf.at[g, :, my_rows, :]
        away = (chip == 3) & (g == 0)
        yield jnp.logical_not(away), [
            remote(qst.at[g], mine, q_send.at[g, 0], q_recv.at[g, core], chip, other)]
        there = qbuf.at[GROUPS, :, my_rows, :]
        yield away, [
            remote(mine, there, q_send.at[g, 1], q_recv.at[GROUPS, core], up, core),
            remote(qst.at[g], there, q_send.at[g, 0], q_recv.at[GROUPS, core], up, other)]

    @pl.loop(0, GROUPS)
    def _(g):
        @pl.when(g == GROUPS - 1)
        def _():
            @pl.when(chip == 1)
            def _():
                wait_straight(2, 0)
                pass_on(2, 0, 0, 1).start()

            @pl.when(chip == 2)
            def _():
                wait_straight(1, 1)
                pass_on(1, 1, 3, 0).start()
                for copy in late_pair():
                    copy.start()

            @pl.when(chip == 3)
            def _():
                wait_straight(0, 1)
                pass_on(0, 1, 2, 0).start()

        with jax.named_scope("q_wait"):
            wide_load(wq_hbm, g, wqsem).wait()
        with jax.named_scope("q_proj"):
            heads = []
            for n in range(3):
                cols = pl.ds(pl.multiple_of(g * 768 + n * 256, 256), 256)
                u = ((matmul_halves if n == 2 else matmul_whole)(hbuf, wbuf[g, :, n * 256 : (n + 1) * 256]) + bq_ref[cols].astype(F32)[None]).astype(BF16)
                heads += [rope(part) for part in lane_blocks(u)]
            for r in range(REPS):
                even, odd = heads[r], heads[REPS + r]
                qbuf[g, r, my_rows, :] = jnp.where(core == 0, even, odd)
                qst[g, r] = jnp.where(core == 0, odd, even)
        wide_load(wo_hbm, g, wosem).start()
        each(q_copies(g), lambda copy: copy.start())

    def masked_item(q_slot, slot, s, g):
        tiles = [(r, slice(start, start + TILE)) for r in range(REPS) for start in range(0, block, TILE)]

        def score(t):
            r, at = tiles[t]
            sc = matmul_t(kv[s, g, 0, 0 : at.stop, :], qbuf[q_slot, r, at, :])
            seen = lax.broadcasted_iota(jnp.int32, (TILE, TILE), 0) <= lax.broadcasted_iota(jnp.int32, (TILE, TILE), 1)
            last = jnp.where(seen, sc[at.start :], -jnp.inf)
            return last if at.start == 0 else jnp.concatenate([sc[: at.start], last], axis=0)

        def soft(t, sc):
            r, at = tiles[t]
            parts = row_blocks(sc)
            top = jnp.max(functools.reduce(jnp.maximum, parts), axis=0, keepdims=True) * SCORE_SCALE
            top = jnp.broadcast_to(top, (8, TILE))
            probs = [jnp.exp2(part * SCORE_SCALE - top) for part in parts]
            run_max[slot, r, :, at] = top
            run_sum[slot, r, :, at] = functools.reduce(jnp.add, probs)
            return (jnp.concatenate(probs, axis=0).astype(BF16),)

        def mix(t, probs):
            r, at = tiles[t]
            mixed[slot, r, :, at] = matmul_tn(kv[s, g, 1, 0 : at.stop, :], probs)

        pipelined(len(tiles), score, soft, mix)

    def full_item(q_slot, slot, s, g):
        def score(r):
            return matmul_t(kv[s, g, 0], qbuf[q_slot, r])

        def soft(r, sc):
            parts = row_blocks(sc)
            before = run_max[slot, r]
            top = jnp.max(functools.reduce(jnp.maximum, parts), axis=0, keepdims=True) * SCORE_SCALE
            top = jnp.maximum(before, top)
            rescale = jnp.exp2(before - top)
            probs = [jnp.exp2(part * SCORE_SCALE - top) for part in parts]
            run_max[slot, r] = top
            run_sum[slot, r] = run_sum[slot, r] * rescale + functools.reduce(jnp.add, probs)
            return jnp.concatenate(probs, axis=0).astype(BF16), rescale

        def mix(r, probs, rescale):
            mixed[slot, r] = mixed[slot, r] * rescale[0:1] + matmul_tn(kv[s, g, 1], probs)

        pipelined(REPS, score, soft, mix)

    def head_cols(g, parity):
        return pl.ds(pl.multiple_of((2 * g + parity) * REPS * 128, 128), REPS * 128)

    def normalized(slot, r, rows):
        total = jnp.sum(run_sum[slot, r, :, rows], axis=0, keepdims=True)
        return jnp.transpose(mixed[slot, r, :, rows] / total).astype(BF16)

    def o_copy(g):
        return remote(ost.at[g], obuf.at[:, head_cols(g, core)], o_send.at[g], o_recv.at[g, core], chip, other)

    def finish(g):
        for r in range(REPS):
            ost[g, :, r * 128 : (r + 1) * 128] = normalized(g, r, other_rows)
        o_copy(g).start()
        for r in range(REPS):
            cols = pl.ds(pl.multiple_of(((2 * g + core) * REPS + r) * 128, 128), 128)
            obuf[:, cols] = normalized(g, r, my_rows)

    def back_copies():
        for j in range(2):
            yield remote(ost.at[GROUPS + j], obuf.at[:, head_cols(0, core)], o_send.at[GROUPS + j], o_recv.at[0, core], down, j)

    low = jnp.where(chip == 3, 1, 0)

    @pl.loop(low, jnp.where(chip == 0, GROUPS + 1, GROUPS))
    def _(i):
        g = lax.rem(i, GROUPS)

        @pl.when(i < GROUPS)
        def _():
            part = qbuf.at[i, :, other_rows, :]
            pltpu.make_async_copy(part, part, q_recv.at[i, other]).wait()
            part = kv.at[chip, g, :, other_rows, :]
            pltpu.make_async_copy(part, part, kv_recv.at[chip, g, other]).wait()

        @pl.when(i == GROUPS)
        def _():
            wait_straight(1, 3)
            pass_on(1, 3, 3, 0).start()
            wait_straight(3, 0)
            for j in range(2):
                part = qbuf.at[GROUPS, :, pl.ds(j * tokens, tokens), :]
                pltpu.make_async_copy(part, part, q_recv.at[GROUPS, j]).wait()

        with jax.named_scope('masked'):
            masked_item(i, g, jnp.where(i == GROUPS, 3, chip), g)

        @pl.when((chip == 0) & (i < GROUPS))
        def _():
            finish(i)

    def wait_o(g, parity):
        part = obuf.at[:, head_cols(g, parity)]
        pltpu.make_async_copy(part, part, o_recv.at[g, parity]).wait()

    def out_parts(n):
        for part in range(3):
            yield part, pl.ds(pl.multiple_of(n * 768 + part * 256, 256), 256)

    def out_product(n, part, g):
        at = pl.ds(pl.multiple_of(g * 768, 256), 768)
        return (matmul_halves if part == 2 else matmul_whole)(obuf.at[:, at], wbuf[n, at, part * 256 : (part + 1) * 256])

    tables = (
        ((0, 1, 2, 4, 5), (0, 0, 0, 1, 3)),
        ((0, 0, 0, 0, 4, 5), (1, 0, 2, 3, 1, 3)),
        ((1, 1, 0, 1, 0, 4, 1, 5, 0, 0), (1, 0, 1, 2, 2, 1, 3, 2, 3, 0)),
        ((0, 2, 0, 2, 1, 0, 4, 2, 1, 1, 5), (2, 1, 1, 2, 1, 3, 1, 3, 3, 2, 3)),
    )

    @pl.when(chip == 3)
    def _():
        for copy in late_pair():
            copy.start()

    @pl.loop(0, pick(chip, [len(sources) for sources, _ in tables]))
    def _(i):
        s = pick(chip, [pick(i, sources) for sources, _ in tables])
        g = pick(chip, [pick(i, groups) for _, groups in tables])
        @pl.when(s < CHIPS)
        def _():
            q_slot = jnp.where(chip == 0, GROUPS, g)
            is_passed = ((chip == 0) & (s == 2)) | ((chip == 2) & (s == 0)) | ((chip == 3) & (s == 1))
            is_here = ((chip == 0) & (s == 0)) | ((chip == 2) & (s == 1) & (g == 1)) | ((chip == 3) & (s == 0) & ((g == 1) | (g == 3)))

            with jax.named_scope("item_wait"):
                @pl.when(is_passed)
                def _():
                    wait_passed(s, g)

                @pl.when(jnp.logical_not(is_passed | is_here))
                def _():
                    wait_straight(s, g)

            @pl.when((chip == 1) & (g == 0))
            def _():
                pass_on(0, 0, 2, 0).start()

            @pl.when((chip == 2) & (s == 1) & (g == 2))
            def _():
                pass_on(1, 2, 3, 1).start()

            @pl.when((chip == 3) & (s == 0) & (g == 2))
            def _():
                pass_on(0, 2, 2, 1).start()

            @pl.when((chip == 3) & (s == 2) & (g == 2))
            def _():
                wait_straight(0, 3)
                pass_on(0, 3, 2, 2).start()

            with jax.named_scope('full'):
                full_item(q_slot, g, s, g)

            @pl.when((chip == 1) | ((chip == 2) & (s == 0)) | ((chip == 3) & (s == 1)))
            def _():
                finish(g)

            @pl.when((chip == 0) & (s == 2))
            def _():
                for j in range(2):
                    rows = pl.ds(j * tokens, tokens)
                    for r in range(REPS):
                        ost[GROUPS + j, :, r * 128 : (r + 1) * 128] = normalized(0, r, rows)
                for copy in back_copies():
                    copy.start()
                wait_straight(3, 1)
                pass_on(3, 1, 1, 1).start()

        @pl.when(s == CHIPS)
        def _():
            wait_o(1, other)

            @pl.loop(0, 4)
            def _(n):
                wide_load(wo_hbm, n, wosem).wait()
                with jax.named_scope("o_proj_a"):
                    for part, cols in out_parts(n):
                        summed[:, cols] = xbuf[:, cols].astype(F32) + out_product(n, part, 1)

        @pl.when(s == CHIPS + 1)
        def _():
            wait_o(g, other)

            @pl.loop(0, 4)
            def _(n):
                with jax.named_scope("o_proj_b"):
                    for part, cols in out_parts(n):
                        summed[:, cols] += out_product(n, part, g)

    @pl.when(chip == 1)
    def _():
        wait_straight(2, 1)
        wait_passed(3, 1)

    @pl.when(chip == 2)
    def _():
        wait_straight(3, 2)

    @pl.loop(0, GROUPS)
    def _(g):
        for kind in range(2):
            each(own_copies(g, kind), lambda copy: copy.wait_send())
        each(q_copies(g), lambda copy: copy.wait_send())

    @pl.loop(low, GROUPS)
    def _(g):
        o_copy(g).wait_send()

    @pl.when(chip == 0)
    def _():
        for copy in back_copies():
            copy.wait_send()

    @pl.when(chip >= 2)
    def _():
        for copy in late_pair():
            copy.wait_send()

    for slot in range(2):
        pass_on(0, 0, up, slot).wait_send()

    @pl.when(chip == 3)
    def _():
        pass_on(0, 0, up, 2).wait_send()

    with jax.named_scope("cache"):
        for s in range(CHIPS):
            for kind, c_ref in ((0, kc_ref), (1, vc_ref)):
                c_ref[s * block : (s + 1) * block, :] = kv[s, chip, kind]

    last_group = jnp.where(chip == 2, 3, 2)
    with jax.named_scope("o_wait"):
        wait_o(last_group, other)

        @pl.when(chip < 3)
        def _():
            wait_o(0, other)

        @pl.when(chip == 3)
        def _():
            for parity in range(2):
                wait_o(0, parity)

    @pl.loop(0, 4)
    def _(n):
        with jax.named_scope("o_proj"):
            for part, cols in out_parts(n):
                y_ref[:, cols] = (summed[:, cols] + (out_product(n, part, 0) + out_product(n, part, last_group))).astype(BF16)


def hand_over(*refs):
    sem = refs[-1]
    count = len(refs) // 2
    copies = []
    for n in range(count):
        rows = refs[n].shape[0] // 2
        for part in range(2):
            at = pl.ds(part * rows, rows)
            copies.append(pltpu.make_async_copy(refs[n].at[at], refs[count + n].at[at], sem.at[n, part]))
    for copy in copies:
        copy.start()
    for copy in copies:
        copy.wait()


def solution(mesh):
    group_size = mesh.shape['sp']
    row_spec = P(('dp', 'sp'), None)
    pos_spec = P(('dp', 'sp'))
    cache_spec = P('dp', 'sp', None)
    whole = P()

    def local(hidden, positions, norm_gain, w_q, b_q, w_k, b_k, w_v, b_v, w_o):
        tokens, width = hidden.shape
        block = 2 * tokens
        seq_len = tokens * group_size
        inv_freq = jnp.asarray(np.float32(ROPE_BASE) ** (np.float32(-2.0) * np.arange(HEAD_DIM // 2, dtype=np.float32) / np.float32(HEAD_DIM)))
        small = (norm_gain, b_q, b_k, b_v)
        anywhere = pl.BlockSpec(memory_space=pl.ANY)
        vmem = pl.BlockSpec(memory_space=pltpu.VMEM)
        dma = pltpu.SemaphoreType.DMA
        y, keys, values = pl.pallas_call(
            kernel,
            out_shape=[
                pltpu.VMEM((tokens, width), BF16),
                pltpu.VMEM((seq_len, HEAD_DIM), BF16),
                pltpu.VMEM((seq_len, HEAD_DIM), BF16),
            ],
            in_specs=[anywhere] * 11,
            out_specs=[vmem] * 3,
            scratch_shapes=[
                pltpu.VMEM((tokens, width), BF16),
                pltpu.VMEM((tokens, width), BF16),
                pltpu.VMEM((tokens,), jnp.int32),
                pltpu.VMEM((HEAD_DIM // 2,), F32),
                *(pltpu.VMEM(a.shape, BF16) for a in small),
                pltpu.VMEM((tokens, HEAD_DIM), F32),
                pltpu.VMEM((tokens, HEAD_DIM), F32),
                pltpu.VMEM((GROUPS, width, 768), BF16),
                pltpu.VMEM((CHIPS, GROUPS, 2, block, HEAD_DIM), BF16),
                pltpu.VMEM((GROUPS, 2, tokens, HEAD_DIM), BF16),
                pltpu.VMEM((GROUPS + 1, REPS, block, HEAD_DIM), BF16),
                pltpu.VMEM((GROUPS, REPS, tokens, HEAD_DIM), BF16),
                pltpu.VMEM((GROUPS, REPS, 8, block), F32),
                pltpu.VMEM((GROUPS, REPS, 8, block), F32),
                pltpu.VMEM((GROUPS, REPS, HEAD_DIM, block), F32),
                pltpu.VMEM((tokens, width), BF16),
                pltpu.VMEM((GROUPS + 2, tokens, REPS * HEAD_DIM), BF16),
                pltpu.VMEM((tokens, width), F32),
                dma((4,)), dma((6,)), dma((GROUPS, 2)), dma((4,)), dma((4,)),
                dma((CHIPS, GROUPS, 2)), dma((GROUPS, 5, 2)), dma((GROUPS + 1, 2)), dma((GROUPS, 2)),
                dma((GROUPS, 2)), dma((GROUPS + 2,)), dma((3,)),
            ],
            compiler_params=pltpu.CompilerParams(
                collective_id=0, has_side_effects=True, vmem_limit_bytes=62500000),
            name="block",
        )(
            hidden, positions, inv_freq, *small, w_q, w_k, w_v, w_o,
        )
        results = [pltpu.with_memory_space_constraint(a, pltpu.VMEM) for a in (y, keys, values)]
        y, keys, values = pl.pallas_call(
            hand_over,
            out_shape=[jax.ShapeDtypeStruct(a.shape, a.dtype) for a in results],
            in_specs=[vmem] * 3,
            out_specs=[anywhere] * 3,
            scratch_shapes=[dma((3, 2))],
            compiler_params=pltpu.CompilerParams(vmem_limit_bytes=1 << 20),
            name="hand_over",
        )(*results)
        return y, keys[:, None, :], values[:, None, :]

    return jax.shard_map(local, mesh=mesh, in_specs=(row_spec, pos_spec, whole, whole, whole, whole, whole, whole, whole, whole), out_specs=(row_spec, cache_spec, cache_spec), check_vma=False)
```
